32 devices in a mesh: dp: 2 (over x), tp: 16 (over y, z, core).
Axes of the slice: x: 2, y: 2, z: 4, core: 2. Of those that a mesh axis runs over, the one named last changes fastest.
Arguments:
- x: bfloat16 [4096, 8192], P(('dp', 'tp')), parts along dimension 0
- gain: bfloat16 [8192], replicated
- wq: bfloat16 [8192, 8192], P(None, 'tp')
- wk: bfloat16 [8192, 8192], P(None, 'tp')
- wv: bfloat16 [8192, 8192], P(None, 'tp')
- wo: bfloat16 [8192, 8192], P('tp')
Outputs:
- output: bfloat16 [4096, 8192], P(('dp', 'tp')), parts along dimension 0
There are 2 independent parts. The reference program is written for one: setup_inputs(seed, part) draws one part's arguments, and reference() takes and returns one part's arrays. A program takes and returns all parts, laid end to end along the dimension named above; an argument that names none is the same for every part.
All inputs are finite; a program needn't handle non-finite values.
Results may differ from the reference program's by a relative error of at most 0.012.
Values are sent between devices in bfloat16 or wider.
A program may use at most 2 GiB of HBM per device.

```python
import jax
import jax.numpy as jnp
from jax import lax

ROWS = 2048
D = 8192
HEADS = 64
KV_HEADS = 64
HEAD = 128
THETA = 10000


def setup_inputs(seed: int = 0, part: int = 0) -> dict:
    kx, kn, kq, kk, kv, ko = jax.random.split(jax.random.key(seed), 6)

    def weights(key, rows, columns):
        return jax.random.normal(key, (rows, columns), jnp.float32) * rows**-0.5

    drawn = {
        "x": jax.random.normal(jax.random.fold_in(kx, part), (ROWS, D), jnp.float32),
        "gain": 1 + 0.1 * jax.random.normal(kn, (D,), jnp.float32),
        "wq": 2 * weights(kq, D, HEADS * HEAD),
        "wk": 2 * weights(kk, D, KV_HEADS * HEAD),
        "wv": 4 * weights(kv, D, KV_HEADS * HEAD),
        "wo": weights(ko, HEADS * HEAD, D),
    }
    return {k: v.astype(jnp.bfloat16) for k, v in drawn.items()}


def normed(x, gain):
    wide = x.astype(jnp.float32)
    scale = lax.rsqrt(jnp.mean(wide * wide, -1, keepdims=True) + 1e-6)
    return (wide * scale * gain.astype(jnp.float32)).astype(jnp.bfloat16)


def turned(t, place, theta):
    half = t.shape[-1] // 2
    angle = place.astype(jnp.float32)[:, None] * theta ** (-jnp.arange(half, dtype=jnp.float32) / half)
    cos, sin = jnp.cos(angle)[:, None], jnp.sin(angle)[:, None]
    a, b = t[..., :half].astype(jnp.float32), t[..., half:].astype(jnp.float32)
    return jnp.concatenate([a * cos - b * sin, b * cos + a * sin], -1).astype(jnp.bfloat16)


def matmul(a, w):
    return jnp.dot(a, w, preferred_element_type=jnp.float32).astype(jnp.bfloat16)


def einsum(form, a, b):
    return jnp.einsum(form, a.astype(jnp.float32), b.astype(jnp.float32))


def attention(q, k, v):
    scores = einsum("tgsd,ugd->gstu", q, k) * q.shape[-1] ** -0.5
    token = jnp.arange(q.shape[0])
    scores = jnp.where(token[:, None] >= token, scores, -jnp.inf)
    weights = jax.nn.softmax(scores, -1).astype(jnp.bfloat16)
    return einsum("gstu,ugd->tgsd", weights, v).astype(jnp.bfloat16)


def reference(x, gain, wq, wk, wv, wo):
    a, place = normed(x, gain), jnp.arange(ROWS)
    q = turned(matmul(a, wq).reshape(ROWS, HEADS, HEAD), place, THETA).reshape(ROWS, KV_HEADS, -1, HEAD)
    k = turned(matmul(a, wk).reshape(ROWS, KV_HEADS, HEAD), place, THETA)
    v = matmul(a, wv).reshape(ROWS, KV_HEADS, HEAD)
    seen = attention(q, k, v).reshape(ROWS, HEADS * HEAD)
    return (x.astype(jnp.float32) + jnp.dot(seen, wo, preferred_element_type=jnp.float32)).astype(jnp.bfloat16)
```

```python
import functools

import jax
import jax.numpy as jnp
import numpy as np
from jax import lax
from jax.experimental import pallas as pl
from jax.experimental.pallas import tpu as pltpu
from jax.sharding import PartitionSpec as P

HEAD = 128
THETA = 10000
NEG = -1e30
HIDDEN = 2 * NEG
LOG2E = 1.4426950408889634
CHIPS = 8
ROWS = 128
SUBS = 4
KEYS = 256
VMEM = 67043328
MESH = pl.DeviceIdType.MESH


def _dot(a, b, ca=1, cb=0):
    return lax.dot_general(a, b, (((ca,), (cb,)), ((), ())), preferred_element_type=jnp.float32)


def _chip(pos):
    return pos + lax.div(pos, 4) * (11 - 2 * pos)


def _where():
    me = lax.axis_index("tp")
    core, chip = lax.rem(me, 2), lax.div(me, 2)
    pos = _chip(chip)
    after = 2 * _chip(lax.rem(pos + 1 + 6 * core, CHIPS)) + core
    before = 2 * _chip(lax.rem(pos + 7 - 6 * core, CHIPS)) + core
    return core, pos, after, before, me + 1 - 2 * core


def _owner(pos, steps, parity):
    return 2 * _chip(lax.rem(pos + steps * (7 - 6 * parity), CHIPS)) + parity


def _meet(devices):
    barrier = pltpu.get_barrier_semaphore()
    for device in devices:
        pl.semaphore_signal(barrier, inc=1, device_id={"tp": device}, device_id_type=MESH)
    return lambda: pl.semaphore_wait(barrier, len(devices))


def _send(src, dst, send_sem, recv_sem, device):
    return pltpu.make_async_remote_copy(src_ref=src, dst_ref=dst, send_sem=send_sem, recv_sem=recv_sem, device_id={"tp": device},
                                        device_id_type=MESH)


def _gather_kernel(x_ref, gain_ref, cos_f, sin_f, cos_c, sin_c, wq_ref, wk_ref, wv_ref, q_ref, k_ref, vt_ref,
                   xs, w_s, acc_s, stage, ring_send, ring_recv, pair_send, pair_recv, w_sem, out_sem):
    core, pos, after, before, partner = _where()
    depth, cols = w_s.shape[1], w_s.shape[2]
    heads = cols // HEAD
    part = ROWS // SUBS
    met = _meet((after, before, partner))
    loads = [pltpu.make_async_copy(w, w_s.at[p], w_sem.at[p]) for p, w in enumerate((wq_ref, wk_ref, wv_ref))]
    for load in loads:
        load.start()

    def rows(s, parity, j):
        return xs.at[s, parity, pl.ds(j * part, part)]

    def ring(s, j):
        return _send(rows(s, core, j), rows(s + 1, core, j), ring_send.at[s, j], ring_recv.at[s, j], after)

    def pair(s, j, parity):
        return _send(rows(s, parity, j), rows(s, parity, j), pair_send.at[s, j], pair_recv.at[s, j], partner)

    for j in range(SUBS):
        for i in range(part // 16):
            here = pl.ds(j * part + 16 * i, 16)
            wide = x_ref[here, :].astype(jnp.float32)
            scale = lax.rsqrt(jnp.sum(wide * wide, -1, keepdims=True) * (1 / depth) + 1e-6)
            xs[0, core, here, :] = (x_ref[here, :].astype(jnp.float32) * scale * gain_ref[...].astype(jnp.float32)).astype(jnp.bfloat16)
        if j == 0:
            met()
        ring(0, j).start()
        pair(0, j, core).start()

    deep = min(depth, 2048)

    def out_copy(p, parity, at):
        if p == 2:
            return pltpu.make_async_copy(stage.at[p, parity], vt_ref.at[:, :, pl.ds(at, ROWS)], out_sem.at[p, parity])
        return pltpu.make_async_copy(stage.at[p, parity], (q_ref, k_ref)[p].at[:, pl.ds(at, ROWS), :], out_sem.at[p, parity])

    def project(s, p):
        @pl.when(s == 0)
        def _():
            loads[p].wait()

        @pl.when(s > 0)
        def _():
            for parity in range(2):
                out_copy(p, parity, 0).wait()

        acc_s[...] = jnp.zeros_like(acc_s)

        def piece(k, _):
            here = pl.ds(pl.multiple_of(k * deep, deep), deep)
            acc_s[...] += _dot(xs[s, :, :, here].reshape(2 * ROWS, deep), w_s[p, here, :])

        lax.fori_loop(0, depth // deep, piece, None)
        for parity in range(2):
            device = _owner(pos, s, parity)
            if p < 2:
                cf, sf, cc, sc = cos_f[...], sin_f[...], cos_c[device], sin_c[device]
                cos, sin = cc * cf - sc * sf, sc * cf + cc * sf
            for h in range(heads):
                t = acc_s[parity * ROWS : (parity + 1) * ROWS, h * HEAD : (h + 1) * HEAD].astype(jnp.bfloat16).astype(jnp.float32)
                t = t * cos + pltpu.roll(t, HEAD // 2, 1) * sin if p < 2 else t.T
                stage[p, parity, h] = t.astype(jnp.bfloat16)
            out_copy(p, parity, pl.multiple_of(device * ROWS, ROWS)).start()

    def step(s, _):
        for j in range(SUBS):
            @pl.when(s < CHIPS)
            def _():
                ring(s - 1, j).wait_recv()

                @pl.when(s < CHIPS - 1)
                def _():
                    ring(s, j).start()

                pair(s, j, core).start()

            if j == 0:
                for i in range(SUBS):
                    pair(s - 1, i, 1 - core).wait_recv()
            if j < 3:
                project(s - 1, j)

    lax.fori_loop(1, CHIPS + 1, step, None)

    def finish(s, _):
        for j in range(SUBS):
            @pl.when(s < CHIPS - 1)
            def _():
                ring(s, j).wait_send()

            pair(s, j, core).wait_send()

    lax.fori_loop(0, CHIPS, finish, None)
    for p in range(3):
        for parity in range(2):
            out_copy(p, parity, 0).wait()


def _tables():
    rate = np.tile(float(THETA) ** (-np.arange(HEAD // 2) / (HEAD // 2)), 2)
    sign = np.where(np.arange(HEAD) < HEAD // 2, -1.0, 1.0)
    fine, coarse = np.arange(ROWS)[:, None] * rate, (np.arange(2 * CHIPS) * ROWS)[:, None, None] * rate
    return [jnp.asarray(t, jnp.float32) for t in (np.cos(fine), np.sin(fine) * sign, np.cos(coarse), np.sin(coarse) * sign)]


def _gather(x, gain, wq, wk, wv):
    depth, cols = wq.shape
    heads, tokens = cols // HEAD, 2 * CHIPS * ROWS
    here, there = pl.BlockSpec(memory_space=pltpu.VMEM), pl.BlockSpec(memory_space=pl.ANY)
    return pl.pallas_call(
        _gather_kernel,
        out_shape=[jax.ShapeDtypeStruct((heads, tokens, HEAD), jnp.bfloat16)] * 2 + [jax.ShapeDtypeStruct((heads, HEAD, tokens), jnp.bfloat16)],
        in_specs=[here] * 6 + [there] * 3,
        out_specs=[there] * 3,
        scratch_shapes=[
            pltpu.VMEM((CHIPS, 2, ROWS, depth), jnp.bfloat16),
            pltpu.VMEM((3, depth, cols), jnp.bfloat16),
            pltpu.VMEM((2 * ROWS, cols), jnp.float32),
            pltpu.VMEM((3, 2, heads, HEAD, HEAD), jnp.bfloat16),
            pltpu.SemaphoreType.DMA((CHIPS - 1, SUBS)),
            pltpu.SemaphoreType.DMA((CHIPS - 1, SUBS)),
            pltpu.SemaphoreType.DMA((CHIPS, SUBS)),
            pltpu.SemaphoreType.DMA((CHIPS, SUBS)),
            pltpu.SemaphoreType.DMA((3,)),
            pltpu.SemaphoreType.DMA((3, 2)),
        ],
        compiler_params=pltpu.CompilerParams(collective_id=0, has_side_effects=True, vmem_limit_bytes=VMEM),
        cost_estimate=pl.CostEstimate(flops=6 * tokens * depth * cols, bytes_accessed=6 * depth * cols, transcendentals=0),
        name="gather_project",
    )(x, gain.reshape(1, -1), *_tables(), wq, wk, wv)


def _scatter_kernel(x_ref, q_ref, k_ref, vt_ref, wo_ref, y_ref, q_s, k_s, v_s, wo_s, run, pin, pout, own, seen, top_s, sum_s, mix_s,
                    ring_send, ring_recv, pair_send, pair_recv, in_sem, wo_sem):
    core, pos, after, before, partner = _where()
    heads, wide = q_s.shape[0], own.shape[2]
    met = _meet((after, before, partner))
    ins = [pltpu.make_async_copy(a, b, in_sem.at[i]) for i, (a, b) in enumerate(((q_ref, q_s), (k_ref, k_s), (vt_ref, v_s)))]
    ins += [pltpu.make_async_copy(wo_ref.at[:, pl.ds(j * wide, wide)], wo_s.at[j], wo_sem.at[j]) for j in range(SUBS)]
    for copy in ins:
        copy.start()
    e = HEAD**-0.5 * LOG2E

    def ring(s, j):
        return _send(run.at[s, j], run.at[s + 1, j], ring_send.at[s, j], ring_recv.at[s, j], after)

    def pair(s, j):
        return _send(pout.at[lax.rem(s, 2), j], pin.at[s, j], pair_send.at[s, j], pair_recv.at[s, j], partner)

    def attend(s, which):
        device = _owner(pos, s + 1, lax.rem(core + which, 2))
        here = pl.ds(pl.multiple_of(device * ROWS, ROWS), ROWS)
        top_s[...] = jnp.full_like(top_s, NEG)
        sum_s[...] = jnp.zeros_like(sum_s)
        mix_s[...] = jnp.zeros_like(mix_s)

        def block(i, masked):
            keys = pl.ds(pl.multiple_of(i * KEYS, KEYS), KEYS)
            scores = [_dot(k_s[h, keys, :], q_s[h, here, :], 1, 1) for h in range(heads)]
            if masked:
                gap = lax.broadcasted_iota(jnp.int32, (KEYS, ROWS), 1) - lax.broadcasted_iota(jnp.int32, (KEYS, ROWS), 0)
                ok = gap >= i * KEYS - device * ROWS
                scores = [jnp.where(ok, t, HIDDEN) for t in scores]
            weights = []
            for h, t in enumerate(scores):
                old = top_s[h]
                top = jnp.maximum(old, t.max(axis=0, keepdims=True))
                p = jnp.exp2((t - top) * e)
                keep = jnp.exp2((old - top) * e)
                top_s[h] = top
                sum_s[h] = sum_s[h] * keep + p.sum(axis=0, keepdims=True)
                weights.append((p.astype(jnp.bfloat16), keep))
            for h, (p, keep) in enumerate(weights):
                mix_s[h] = mix_s[h] * keep + _dot(v_s[h, :, keys], p)

        whole = lax.div(device * ROWS, KEYS)
        lax.fori_loop(0, whole, lambda i, _: block(i, False), None)
        block(whole, True)
        for h in range(heads):
            out = (mix_s[h] * (1 / sum_s[h])).T
            seen[lax.rem(s, 2), which, :, h * HEAD : (h + 1) * HEAD] = out.astype(jnp.bfloat16)

    narrow = min(wide, 512)

    def project(s, j):
        both = seen[lax.rem(s, 2)].reshape(2 * ROWS, heads * HEAD)
        for n in range(0, wide, narrow):
            term = _dot(both, wo_s[j, :, n : n + narrow])
            own[j, :, n : n + narrow] = term[:ROWS]
            pout[lax.rem(s, 2), j, :, n : n + narrow] = term[ROWS:].astype(jnp.bfloat16)
        pair(s, j).start()

    def add(s, j, i, running):
        here = pl.ds(pl.multiple_of(i * 16, 16), 16)
        total = own[j, here, :] + pin[s, j, here, :].astype(jnp.float32)
        return here, total + run[s, j, here, :].astype(jnp.float32) if running else total

    def first(j, _):
        pair(0, j).wait_recv()

        def some(i, _):
            here, total = add(0, j, i, False)
            run[0, j, here, :] = total.astype(jnp.bfloat16)

        lax.fori_loop(0, ROWS // 16, some, None)
        ring(0, j).start()

    for copy in ins[:3]:
        copy.wait()
    lax.fori_loop(0, 2, lambda i, _: attend(0, i), None)
    for copy in ins[3:]:
        copy.wait()
    met()
    lax.fori_loop(0, SUBS, lambda j, _: project(0, j), None)
    lax.fori_loop(0, SUBS, first, None)
    lax.fori_loop(0, 2, lambda i, _: attend(1, i), None)
    lax.fori_loop(0, SUBS, lambda j, _: project(1, j), None)
    lax.fori_loop(0, 2, lambda i, _: attend(2, i), None)

    def turn(t, _):
        s, j = lax.div(t, SUBS), lax.rem(t, SUBS)
        ring(s - 1, j).wait_recv()
        pair(s, j).wait_recv()

        @pl.when(s < CHIPS - 1)
        def _():
            def some(i, _):
                here, total = add(s, j, i, True)
                run[s, j, here, :] = total.astype(jnp.bfloat16)

            lax.fori_loop(0, ROWS // 16, some, None)
            ring(s, j).start()
            pair(s - 1, j).wait_send()
            project(s + 1, j)

        @pl.when(s == CHIPS - 1)
        def _():
            def some(i, _):
                here, total = add(s, j, i, True)
                columns = pl.ds(pl.multiple_of(j * wide, wide), wide)
                y_ref[here, columns] = (x_ref[here, columns].astype(jnp.float32) + total).astype(jnp.bfloat16)

            lax.fori_loop(0, ROWS // 16, some, None)

        @pl.when((s < CHIPS - 2) & (j < 2))
        def _():
            attend(s + 2, j)

    lax.fori_loop(SUBS, CHIPS * SUBS, turn, None)

    def finish(s, _):
        for j in range(SUBS):
            ring(s, j).wait_send()

    lax.fori_loop(0, CHIPS - 1, finish, None)
    for s in (CHIPS - 2, CHIPS - 1):
        for j in range(SUBS):
            pair(s, j).wait_send()


def _scatter(x, q, k, vt, wo):
    cols, depth = wo.shape
    heads, tokens = cols // HEAD, 2 * CHIPS * ROWS
    wide = depth // SUBS
    here, there = pl.BlockSpec(memory_space=pltpu.VMEM), pl.BlockSpec(memory_space=pl.ANY)
    low = jnp.bfloat16
    return pl.pallas_call(
        _scatter_kernel,
        out_shape=jax.ShapeDtypeStruct((ROWS, depth), low),
        in_specs=[here] + [there] * 4,
        out_specs=here,
        scratch_shapes=[
            pltpu.VMEM((heads, tokens, HEAD), low),
            pltpu.VMEM((heads, tokens, HEAD), low),
            pltpu.VMEM((heads, HEAD, tokens), low),
            pltpu.VMEM((SUBS, cols, wide), low),
            pltpu.VMEM((CHIPS, SUBS, ROWS, wide), low),
            pltpu.VMEM((CHIPS, SUBS, ROWS, wide), low),
            pltpu.VMEM((2, SUBS, ROWS, wide), low),
            pltpu.VMEM((SUBS, ROWS, wide), jnp.float32),
            pltpu.VMEM((2, 2, ROWS, cols), low),
            pltpu.VMEM((heads, 1, ROWS), jnp.float32),
            pltpu.VMEM((heads, 1, ROWS), jnp.float32),
            pltpu.VMEM((heads, HEAD, ROWS), jnp.float32),
            pltpu.SemaphoreType.DMA((CHIPS - 1, SUBS)),
            pltpu.SemaphoreType.DMA((CHIPS - 1, SUBS)),
            pltpu.SemaphoreType.DMA((CHIPS, SUBS)),
            pltpu.SemaphoreType.DMA((CHIPS, SUBS)),
            pltpu.SemaphoreType.DMA((3,)),
            pltpu.SemaphoreType.DMA((SUBS,)),
        ],
        compiler_params=pltpu.CompilerParams(collective_id=1, has_side_effects=True, vmem_limit_bytes=VMEM),
        cost_estimate=pl.CostEstimate(flops=2 * tokens * depth * cols, bytes_accessed=2 * depth * cols, transcendentals=heads * tokens * tokens // 2),
        name="attend_scatter",
    )(x, q, k, vt, wo)


def solution(mesh):
    def step(x, gain, wq, wk, wv, wo):
        return _scatter(x, *_gather(x, gain, wq, wk, wv), wo)

    tokens, columns = P(("dp", "tp"), None), P(None, "tp")
    return jax.shard_map(
        step,
        mesh=mesh,
        in_specs=(tokens, P(None), columns, columns, columns, P("tp", None)),
        out_specs=tokens,
        check_vma=False,
    )
```

```python
import functools

import jax
import jax.numpy as jnp
import numpy as np
from jax import lax
from jax.experimental import pallas as pl
from jax.experimental.pallas import tpu as pltpu
from jax.sharding import PartitionSpec as P

HEAD = 128
THETA = 10000
NEG = -1e30
HIDDEN = 2 * NEG
LOG2E = 1.4426950408889634
CHIPS = 8
ROWS = 128
SUBS = 4
SIDE = 512
KEYS = 256
VMEM = 67043328
MESH = pl.DeviceIdType.MESH


def _dot(a, b, ca=1, cb=0):
    return lax.dot_general(a, b, (((ca,), (cb,)), ((), ())), preferred_element_type=jnp.float32)


def _chip(pos):
    return pos + lax.div(pos, 4) * (11 - 2 * pos)


def _where():
    me = lax.axis_index("tp")
    core, chip = lax.rem(me, 2), lax.div(me, 2)
    pos = _chip(chip)
    after = 2 * _chip(lax.rem(pos + 1 + 6 * core, CHIPS)) + core
    before = 2 * _chip(lax.rem(pos + 7 - 6 * core, CHIPS)) + core
    return core, pos, after, before, me + 1 - 2 * core


def _owner(pos, steps, parity):
    return 2 * _chip(lax.rem(pos + steps * (7 - 6 * parity), CHIPS)) + parity


def _meet(devices):
    barrier = pltpu.get_barrier_semaphore()
    for device in devices:
        pl.semaphore_signal(barrier, inc=1, device_id={"tp": device}, device_id_type=MESH)
    return lambda: pl.semaphore_wait(barrier, len(devices))


def _send(src, dst, send_sem, recv_sem, device):
    return pltpu.make_async_remote_copy(src_ref=src, dst_ref=dst, send_sem=send_sem, recv_sem=recv_sem, device_id={"tp": device},
                                        device_id_type=MESH)


def _tables():
    rate = np.tile(float(THETA) ** (-np.arange(HEAD // 2) / (HEAD // 2)), 2)
    sign = np.where(np.arange(HEAD) < HEAD // 2, -1.0, 1.0)
    fine, coarse = np.arange(ROWS)[:, None] * rate, (np.arange(2 * CHIPS) * ROWS)[:, None, None] * rate
    return [jnp.asarray(t, jnp.float32) for t in (np.cos(fine), np.sin(fine) * sign, np.cos(coarse), np.sin(coarse) * sign)]


def _x_unit(s, j):
    return SUBS * s + j


def _x_pair(s, j):
    return 32 + SUBS * lax.rem(s, 4) + j


def _w_unit(p, k):
    return 48 + 16 * p + k


def _wo_unit(n):
    return n


def _run_unit(s, j):
    return 16 + SUBS * s + j


def _in_unit(s, j):
    return 48 + SUBS * s + j


def _out_unit(s, j):
    return 80 + SUBS * lax.rem(s, 2) + j


UNITS = 96


def _kernel(x_ref, gain_ref, cos_f, sin_f, cos_c, sin_c, wq_ref, wk_ref, wv_ref, wo_ref, y_ref,
            mem, q_s, k_s, v_s, own, seen, top_s, sum_s, mix_s,
            ring_send, ring_recv, pair_send, pair_recv, sum_send, sum_recv, term_send, term_recv, x_sem, w_sem, wo_sem, credit, phase):
    core, pos, after, before, partner = _where()
    depth = y_ref.shape[1]
    heads = q_s.shape[0]
    wide = depth // SUBS
    parts = wide // SIDE
    met = _meet((after, before, partner))
    x_load = pltpu.make_async_copy(x_ref, y_ref, x_sem)
    x_load.start()
    weights = (wq_ref, wk_ref, wv_ref)

    def w_load(p, j):
        return pltpu.make_async_copy(weights[p].at[pl.ds(parts * j, parts)], mem.at[pl.ds(_w_unit(p, parts * j), parts)], w_sem.at[p, j])

    for j in range(SUBS):
        for p in range(3):
            w_load(p, j).start()

    def ring(s, j):
        return _send(mem.at[_x_unit(s, j)], mem.at[_x_unit(s + 1, j)], ring_send.at[s, j], ring_recv.at[s, j], after)

    def pair(s, j):
        return _send(mem.at[_x_unit(s, j)], mem.at[_x_pair(s, j)], pair_send.at[s, j], pair_recv.at[s, j], partner)

    for n in range(6):
        own[n] = jnp.zeros_like(own[n])
    x_load.wait()
    group = 16
    scales = []
    for r in range(0, ROWS, group):
        wide_x = y_ref[r : r + group, :].astype(jnp.float32)
        scales.append(lax.rsqrt(jnp.sum(wide_x * wide_x, -1, keepdims=True) * (1 / depth) + 1e-6))
    for j in range(SUBS):
        for i in range(parts):
            here = slice(j * wide + i * SIDE, j * wide + (i + 1) * SIDE)
            gain = gain_ref[:, here].astype(jnp.float32)
            for r in range(0, ROWS, group):
                t = y_ref[r : r + group, here].astype(jnp.float32) * scales[r // group] * gain
                mem[_x_unit(0, j), i * ROWS + r : i * ROWS + r + group, :] = t.astype(jnp.bfloat16)
        if j == 0:
            met()
        ring(0, j).start()
        pair(0, j).start()

    def project(t):
        s, j = lax.div(t, SUBS), lax.rem(t, SUBS)
        pair(s, j).wait_recv()
        mine, theirs = _x_unit(s, j), _x_pair(s, j)
        units = mine + core * (theirs - mine), theirs + core * (mine - theirs)
        a = [jnp.concatenate([mem[u, i * ROWS : (i + 1) * ROWS, :] for i in range(parts)], axis=1) for u in units]
        a = jnp.concatenate(a, axis=0)
        for p in range(3):
            @pl.when(s == 0)
            def _():
                w_load(p, j).wait()

            part = _dot(a, mem[pl.ds(_w_unit(p, parts * j), parts)].reshape(wide, SIDE))
            own[p] += part[:ROWS]
            own[3 + p] += part[ROWS:]

        @pl.when(j == SUBS - 1)
        def _():
            for parity in range(2):
                device = _owner(pos, s, parity)
                here = pl.ds(pl.multiple_of(device * ROWS, ROWS), ROWS)
                cf, sf, cc, sc = cos_f[...], sin_f[...], cos_c[device], sin_c[device]
                cos, sin = cc * cf - sc * sf, sc * cf + cc * sf
                for p in range(3):
                    for h in range(heads):
                        t = own[3 * parity + p, :, h * HEAD : (h + 1) * HEAD].astype(jnp.bfloat16).astype(jnp.float32)
                        if p < 2:
                            (q_s, k_s)[p][h, here, :] = (t * cos + pltpu.roll(t, HEAD // 2, 1) * sin).astype(jnp.bfloat16)
                        else:
                            v_s[h, :, here] = t.T.astype(jnp.bfloat16)
            for n in range(6):
                own[n] = jnp.zeros_like(own[n])

            @pl.when(s < 4)
            def _():
                pl.semaphore_signal(credit, inc=1, device_id={"tp": partner}, device_id_type=MESH)

    def wo_load(j):
        return [pltpu.make_async_copy(wo_ref.at[:, pl.ds((parts * j + i) * SIDE, SIDE)], mem.at[_wo_unit(parts * j + i)], wo_sem.at[j, i])
                for i in range(parts)]

    def gather(t, _):
        @pl.when((t >= SUBS) & (t < CHIPS * SUBS))
        def _():
            s, j = lax.div(t, SUBS), lax.rem(t, SUBS)
            ring(s - 1, j).wait_recv()

            @pl.when(s < CHIPS - 1)
            def _():
                ring(s, j).start()

            @pl.when((s >= 4) & (j == 0))
            def _():
                pl.semaphore_wait(credit, 1)

            pair(s, j).start()

        project(t - 1)

        @pl.when(t == 6 * SUBS)
        def _():
            def sent(s, _):
                for j in range(SUBS):
                    ring(s, j).wait_send()
                    pair(s, j).wait_send()

            lax.fori_loop(0, 4, sent, None)
            for j in range(SUBS):
                for load in wo_load(j):
                    load.start()

    lax.fori_loop(1, CHIPS * SUBS + 1, gather, None)

    def sent(s, _):
        for j in range(SUBS):
            @pl.when(s < CHIPS - 1)
            def _():
                ring(s, j).wait_send()

            pair(s, j).wait_send()

    lax.fori_loop(4, CHIPS, sent, None)
    for device in (after, before, partner):
        pl.semaphore_signal(phase, inc=1, device_id={"tp": device}, device_id_type=MESH)
    x_load.start()
    e = HEAD**-0.5 * LOG2E

    def total(s, j):
        return _send(mem.at[_run_unit(s, j)], mem.at[_run_unit(s + 1, j)], sum_send.at[s, j], sum_recv.at[s, j], after)

    def term(s, j):
        return _send(mem.at[_out_unit(s, j)], mem.at[_in_unit(s, j)], term_send.at[s, j], term_recv.at[s, j], partner)

    def attend(s, which):
        device = _owner(pos, s + 1, lax.rem(core + which, 2))
        here = pl.ds(pl.multiple_of(device * ROWS, ROWS), ROWS)
        top_s[...] = jnp.full_like(top_s, NEG)
        sum_s[...] = jnp.zeros_like(sum_s)
        mix_s[...] = jnp.zeros_like(mix_s)

        def block(i, masked):
            keys = pl.ds(pl.multiple_of(i * KEYS, KEYS), KEYS)
            scores = [_dot(k_s[h, keys, :], q_s[h, here, :], 1, 1) for h in range(heads)]
            if masked:
                gap = lax.broadcasted_iota(jnp.int32, (KEYS, ROWS), 1) - lax.broadcasted_iota(jnp.int32, (KEYS, ROWS), 0)
                ok = gap >= i * KEYS - device * ROWS
                scores = [jnp.where(ok, t, HIDDEN) for t in scores]
            weights = []
            for h, t in enumerate(scores):
                old = top_s[h]
                top = jnp.maximum(old, t.max(axis=0, keepdims=True))
                p = jnp.exp2((t - top) * e)
                keep = jnp.exp2((old - top) * e)
                top_s[h] = top
                sum_s[h] = sum_s[h] * keep + p.sum(axis=0, keepdims=True)
                weights.append((p.astype(jnp.bfloat16), keep))
            for h, (p, keep) in enumerate(weights):
                mix_s[h] = mix_s[h] * keep + _dot(v_s[h, :, keys], p)

        whole = lax.div(device * ROWS, KEYS)
        lax.fori_loop(0, whole, lambda i, _: block(i, False), None)
        block(whole, True)
        for h in range(heads):
            out = (mix_s[h] * (1 / sum_s[h])).T
            seen[lax.rem(s, 2), which, :, h * HEAD : (h + 1) * HEAD] = out.astype(jnp.bfloat16)

    def terms(s, j):
        both = seen[lax.rem(s, 2)].reshape(2 * ROWS, heads * HEAD)
        for i in range(parts):
            t = _dot(both, mem[_wo_unit(parts * j + i)])
            own[parts * j + i] = t[:ROWS]
            mem[_out_unit(s, j), i * ROWS : (i + 1) * ROWS, :] = t[ROWS:].astype(jnp.bfloat16)
        term(s, j).start()

    strip = 64

    def add(s, j, running, last):
        def some(g, _):
            i, r = lax.div(g, ROWS // strip), pl.multiple_of(lax.rem(g, ROWS // strip) * strip, strip)
            here = pl.ds(pl.multiple_of(g * strip, strip), strip)
            t = own[parts * j + i, pl.ds(r, strip), :] + mem[_in_unit(s, j), here, :].astype(jnp.float32)
            if running:
                t = t + mem[_run_unit(s, j), here, :].astype(jnp.float32)
            if last:
                columns = pl.ds(pl.multiple_of(j * wide + i * SIDE, SIDE), SIDE)
                y_ref[pl.ds(r, strip), columns] = (y_ref[pl.ds(r, strip), columns].astype(jnp.float32) + t).astype(jnp.bfloat16)
            else:
                mem[_run_unit(s, j), here, :] = t.astype(jnp.bfloat16)

        lax.fori_loop(0, parts * ROWS // strip, some, None)

    def first(j, _):
        term(0, j).wait_recv()
        add(0, j, False, False)
        total(0, j).start()

    lax.fori_loop(0, 2, lambda i, _: attend(0, i), None)
    for j in range(SUBS):
        for load in wo_load(j):
            load.wait()
    pl.semaphore_wait(phase, 3)
    lax.fori_loop(0, SUBS, lambda j, _: terms(0, j), None)
    lax.fori_loop(0, SUBS, first, None)
    lax.fori_loop(0, 2, lambda i, _: attend(1, i), None)
    lax.fori_loop(0, SUBS, lambda j, _: terms(1, j), None)
    lax.fori_loop(0, 2, lambda i, _: attend(2, i), None)
    x_load.wait()

    def scatter(t, _):
        s, j = lax.div(t, SUBS), lax.rem(t, SUBS)
        total(s - 1, j).wait_recv()
        term(s, j).wait_recv()

        @pl.when(s < CHIPS - 1)
        def _():
            add(s, j, True, False)
            total(s, j).start()
            term(s - 1, j).wait_send()
            terms(s + 1, j)

        @pl.when(s == CHIPS - 1)
        def _():
            add(s, j, True, True)

        @pl.when((s < CHIPS - 2) & (j < 2))
        def _():
            attend(s + 2, j)

    lax.fori_loop(SUBS, CHIPS * SUBS, scatter, None)

    def done(s, _):
        for j in range(SUBS):
            total(s, j).wait_send()

    lax.fori_loop(0, CHIPS - 1, done, None)
    for s in (CHIPS - 2, CHIPS - 1):
        for j in range(SUBS):
            term(s, j).wait_send()


def solution(mesh):
    def step(x, gain, wq, wk, wv, wo):
        depth, cols = wq.shape
        heads, tokens = cols // HEAD, 2 * CHIPS * ROWS
        here, there = pl.BlockSpec(memory_space=pltpu.VMEM), pl.BlockSpec(memory_space=pl.ANY)
        low = jnp.bfloat16
        return pl.pallas_call(
            _kernel,
            out_shape=jax.ShapeDtypeStruct((ROWS, depth), low),
            in_specs=[there] + [here] * 5 + [there] * 4,
            out_specs=here,
            scratch_shapes=[
                pltpu.VMEM((UNITS, SIDE, SIDE), low),
                pltpu.VMEM((heads, tokens, HEAD), low),
                pltpu.VMEM((heads, tokens, HEAD), low),
                pltpu.VMEM((heads, HEAD, tokens), low),
                pltpu.VMEM((depth // SIDE, ROWS, SIDE), jnp.float32),
                pltpu.VMEM((2, 2, ROWS, cols), low),
                pltpu.VMEM((heads, 1, ROWS), jnp.float32),
                pltpu.VMEM((heads, 1, ROWS), jnp.float32),
                pltpu.VMEM((heads, HEAD, ROWS), jnp.float32),
                *[pltpu.SemaphoreType.DMA((CHIPS - 1, SUBS))] * 2,
                *[pltpu.SemaphoreType.DMA((CHIPS, SUBS))] * 2,
                *[pltpu.SemaphoreType.DMA((CHIPS - 1, SUBS))] * 2,
                *[pltpu.SemaphoreType.DMA((CHIPS, SUBS))] * 2,
                pltpu.SemaphoreType.DMA,
                pltpu.SemaphoreType.DMA((3, SUBS)),
                pltpu.SemaphoreType.DMA((SUBS, depth // SUBS // SIDE)),
                pltpu.SemaphoreType.REGULAR,
                pltpu.SemaphoreType.REGULAR,
            ],
            compiler_params=pltpu.CompilerParams(collective_id=0, has_side_effects=True, vmem_limit_bytes=VMEM),
            cost_estimate=pl.CostEstimate(flops=8 * tokens * depth * cols, bytes_accessed=8 * depth * cols,
                                          transcendentals=heads * tokens * tokens // 2),
            name="attention_half",
        )(x, gain.reshape(1, -1), *_tables(), *[w.reshape(-1, SIDE, cols) for w in (wq, wk, wv)], wo)

    tokens, columns = P(("dp", "tp"), None), P(None, "tp")
    return jax.shard_map(
        step,
        mesh=mesh,
        in_specs=(tokens, P(None), columns, columns, columns, P("tp", None)),
        out_specs=tokens,
        check_vma=False,
    )
```

```python
import functools

import jax
import jax.numpy as jnp
import numpy as np
from jax import lax
from jax.experimental import pallas as pl
from jax.experimental.pallas import tpu as pltpu
from jax.sharding import PartitionSpec as P

HEAD = 128
THETA = 10000
NEG = -1e30
HIDDEN = 2 * NEG
LOG2E = 1.4426950408889634
CHIPS = 8
ROWS = 128
SUBS = 4
SIDE = 512
KEYS = 256
VMEM = 67043328
MESH = pl.DeviceIdType.MESH


def _dot(a, b, ca=1, cb=0):
    return lax.dot_general(a, b, (((ca,), (cb,)), ((), ())), preferred_element_type=jnp.float32)


def _chip(pos):
    return pos + lax.div(pos, 4) * (11 - 2 * pos)


def _where():
    me = lax.axis_index("tp")
    core, chip = lax.rem(me, 2), lax.div(me, 2)
    pos = _chip(chip)
    after = 2 * _chip(lax.rem(pos + 1 + 6 * core, CHIPS)) + core
    before = 2 * _chip(lax.rem(pos + 7 - 6 * core, CHIPS)) + core
    return core, pos, after, before, me + 1 - 2 * core


def _owner(pos, steps, parity):
    return 2 * _chip(lax.rem(pos + steps * (7 - 6 * parity), CHIPS)) + parity


def _meet(devices):
    barrier = pltpu.get_barrier_semaphore()
    for device in devices:
        pl.semaphore_signal(barrier, inc=1, device_id={"tp": device}, device_id_type=MESH)
    return lambda: pl.semaphore_wait(barrier, len(devices))


def _send(src, dst, send_sem, recv_sem, device):
    return pltpu.make_async_remote_copy(src_ref=src, dst_ref=dst, send_sem=send_sem, recv_sem=recv_sem, device_id={"tp": device},
                                        device_id_type=MESH)


def _tables():
    rate = np.tile(float(THETA) ** (-np.arange(HEAD // 2) / (HEAD // 2)), 2)
    sign = np.where(np.arange(HEAD) < HEAD // 2, -1.0, 1.0)
    fine, coarse = np.arange(ROWS)[:, None] * rate, (np.arange(2 * CHIPS) * ROWS)[:, None, None] * rate
    return [jnp.asarray(t, jnp.float32) for t in (np.cos(fine), np.sin(fine) * sign, np.cos(coarse), np.sin(coarse) * sign)]


def _x_unit(s, j):
    return SUBS * s + j


def _x_pair(s, j):
    return 32 + SUBS * lax.rem(s, 4) + j


def _w_unit(p, k):
    return 48 + 16 * p + k


def _wo_unit(n):
    return n


def _run_unit(s, j):
    return 16 + SUBS * s + j


def _in_unit(s, j):
    return 48 + SUBS * s + j


def _out_unit(s, j):
    return 80 + SUBS * lax.rem(s, 2) + j


UNITS = 96


def _kernel(x_ref, gain_ref, cos_f, sin_f, cos_c, sin_c, wq_ref, wk_ref, wv_ref, wo_ref, out_ref,
            mem, y_s, q_s, k_s, v_s, own, seen, top_s, sum_s, mix_s,
            ring_send, ring_recv, pair_send, pair_recv, sum_send, sum_recv, term_send, term_recv, x_sem, y_sem, w_sem, wo_sem, credit, phase):
    core, pos, after, before, partner = _where()
    depth = y_s.shape[1]
    heads = q_s.shape[0]
    wide = depth // SUBS
    parts = wide // SIDE
    met = _meet((after, before, partner))
    x_load = pltpu.make_async_copy(x_ref, y_s, x_sem)
    x_load.start()
    weights = (wq_ref, wk_ref, wv_ref)

    def w_load(p, j):
        return pltpu.make_async_copy(weights[p].at[pl.ds(parts * j, parts)], mem.at[pl.ds(_w_unit(p, parts * j), parts)], w_sem.at[p, j])

    def ring(s, j):
        return _send(mem.at[_x_unit(s, j)], mem.at[_x_unit(s + 1, j)], ring_send.at[s, j], ring_recv.at[s, j], after)

    def pair(s, j):
        return _send(mem.at[_x_unit(s, j)], mem.at[_x_pair(s, j)], pair_send.at[s, j], pair_recv.at[s, j], partner)

    e = HEAD**-0.5 * LOG2E

    def attend_keys(which, device, start, size, masked):
        here = pl.ds(pl.multiple_of(device * ROWS, ROWS), ROWS)
        keys = pl.ds(pl.multiple_of(start, size), size)
        scores = [_dot(k_s[h, keys, :], q_s[h, here, :], 1, 1) for h in range(heads)]
        if masked:
            gap = lax.broadcasted_iota(jnp.int32, (size, ROWS), 1) - lax.broadcasted_iota(jnp.int32, (size, ROWS), 0)
            ok = gap >= start - device * ROWS
            scores = [jnp.where(ok, t, HIDDEN) for t in scores]
        weights = []
        for h, t in enumerate(scores):
            old = top_s[which, h]
            top = jnp.maximum(old, t.max(axis=0, keepdims=True))
            p = jnp.exp2((t - top) * e)
            keep = jnp.exp2((old - top) * e)
            top_s[which, h] = top
            sum_s[which, h] = sum_s[which, h] * keep + p.sum(axis=0, keepdims=True)
            weights.append((p.astype(jnp.bfloat16), keep))
        for h, (p, keep) in enumerate(weights):
            mix_s[which, h] = mix_s[which, h] * keep + _dot(v_s[h, :, keys], p)

    def begin(which):
        top_s[which] = jnp.full(top_s.shape[1:], NEG, jnp.float32)
        sum_s[which] = jnp.zeros(sum_s.shape[1:], jnp.float32)
        mix_s[which] = jnp.zeros(mix_s.shape[1:], jnp.float32)

    def finish(s, which):
        for h in range(heads):
            out = (mix_s[which, h] * (1 / sum_s[which, h])).T
            seen[lax.rem(s, 2), which, :, h * HEAD : (h + 1) * HEAD] = out.astype(jnp.bfloat16)

    def block_of(s, which):
        return _owner(pos, s + 1, lax.rem(core + which, 2))

    def attend(s, which):
        device = block_of(s, which)
        begin(which)
        whole = lax.div(device * ROWS, KEYS)
        lax.fori_loop(0, whole, lambda i, _: attend_keys(which, device, i * KEYS, KEYS, False), None)
        attend_keys(which, device, whole * KEYS, KEYS, True)
        finish(s, which)

    def ahead(s):
        def some(i, _):
            which, keys = lax.div(i, 2), _owner(pos, s, lax.rem(i, 2))
            device = block_of(0, which)

            @pl.when(keys <= device)
            def _():
                attend_keys(which, device, keys * ROWS, ROWS, True)

        lax.fori_loop(0, 4, some, None)

    for n in range(6):
        own[n] = jnp.zeros_like(own[n])
    for which in range(2):
        begin(which)
    x_load.wait()
    for j in range(SUBS):
        for p in range(3):
            w_load(p, j).start()
    group = 16
    scales = []
    for r in range(0, ROWS, group):
        wide_x = y_s[r : r + group, :].astype(jnp.float32)
        scales.append(lax.rsqrt(jnp.sum(wide_x * wide_x, -1, keepdims=True) * (1 / depth) + 1e-6))
    for j in range(SUBS):
        for i in range(parts):
            here = slice(j * wide + i * SIDE, j * wide + (i + 1) * SIDE)
            gain = gain_ref[here].astype(jnp.float32).reshape(1, SIDE)
            for r in range(0, ROWS, group):
                t = y_s[r : r + group, here].astype(jnp.float32) * scales[r // group] * gain
                mem[_x_unit(0, j), i * ROWS + r : i * ROWS + r + group, :] = t.astype(jnp.bfloat16)
        if j == 0:
            met()
        ring(0, j).start()
        pair(0, j).start()

    def project(t):
        s, j = lax.div(t, SUBS), lax.rem(t, SUBS)
        pair(s, j).wait_recv()
        mine, theirs = _x_unit(s, j), _x_pair(s, j)
        units = mine + core * (theirs - mine), theirs + core * (mine - theirs)
        a = [jnp.concatenate([mem[u, i * ROWS : (i + 1) * ROWS, :] for i in range(parts)], axis=1) for u in units]
        a = jnp.concatenate(a, axis=0)
        for p in range(3):
            @pl.when(s == 0)
            def _():
                w_load(p, j).wait()

            part = _dot(a, mem[pl.ds(_w_unit(p, parts * j), parts)].reshape(wide, SIDE))
            own[p] += part[:ROWS]
            own[3 + p] += part[ROWS:]

        @pl.when(j == SUBS - 1)
        def _():
            for parity in range(2):
                device = _owner(pos, s, parity)
                here = pl.ds(pl.multiple_of(device * ROWS, ROWS), ROWS)
                cf, sf, cc, sc = cos_f[...], sin_f[...], cos_c[device], sin_c[device]
                cos, sin = cc * cf - sc * sf, sc * cf + cc * sf
                for p in range(3):
                    for h in range(heads):
                        t = own[3 * parity + p, :, h * HEAD : (h + 1) * HEAD].astype(jnp.bfloat16).astype(jnp.float32)
                        if p < 2:
                            (q_s, k_s)[p][h, here, :] = (t * cos + pltpu.roll(t, HEAD // 2, 1) * sin).astype(jnp.bfloat16)
                        else:
                            v_s[h, :, here] = t.T.astype(jnp.bfloat16)
            for n in range(6):
                own[n] = jnp.zeros_like(own[n])

            @pl.when(s < 4)
            def _():
                pl.semaphore_signal(credit, inc=1, device_id={"tp": partner}, device_id_type=MESH)

            @pl.when(s == 1)
            def _():
                ahead(0)

            @pl.when(s >= 1)
            def _():
                ahead(s)

    def wo_load(j):
        return [pltpu.make_async_copy(wo_ref.at[:, pl.ds((parts * j + i) * SIDE, SIDE)], mem.at[_wo_unit(parts * j + i)], wo_sem.at[j, i])
                for i in range(parts)]

    def gather(t, _):
        @pl.when((t >= SUBS) & (t < CHIPS * SUBS))
        def _():
            s, j = lax.div(t, SUBS), lax.rem(t, SUBS)
            ring(s - 1, j).wait_recv()

            @pl.when(s < CHIPS - 1)
            def _():
                ring(s, j).start()

            @pl.when((s >= 4) & (j == 0))
            def _():
                pl.semaphore_wait(credit, 1)

            pair(s, j).start()

        project(t - 1)

        @pl.when(t == 6 * SUBS)
        def _():
            def sent(s, _):
                for j in range(SUBS):
                    ring(s, j).wait_send()
                    pair(s, j).wait_send()

            lax.fori_loop(0, 4, sent, None)
            for j in range(SUBS):
                for load in wo_load(j):
                    load.start()

    lax.fori_loop(1, CHIPS * SUBS + 1, gather, None)

    def sent(s, _):
        for j in range(SUBS):
            @pl.when(s < CHIPS - 1)
            def _():
                ring(s, j).wait_send()

            pair(s, j).wait_send()

    lax.fori_loop(4, CHIPS, sent, None)
    for device in (after, before, partner):
        pl.semaphore_signal(phase, inc=1, device_id={"tp": device}, device_id_type=MESH)
    x_load.start()
    def total(s, j):
        return _send(mem.at[_run_unit(s, j)], mem.at[_run_unit(s + 1, j)], sum_send.at[s, j], sum_recv.at[s, j], after)

    def term(s, j):
        return _send(mem.at[_out_unit(s, j)], mem.at[_in_unit(s, j)], term_send.at[s, j], term_recv.at[s, j], partner)

    def terms(s, j):
        both = seen[lax.rem(s, 2)].reshape(2 * ROWS, heads * HEAD)
        for i in range(parts):
            t = _dot(both, mem[_wo_unit(parts * j + i)])
            own[parts * j + i] = t[:ROWS]
            mem[_out_unit(s, j), i * ROWS : (i + 1) * ROWS, :] = t[ROWS:].astype(jnp.bfloat16)
        term(s, j).start()

    strip = 64

    def add(s, j, running, last):
        def some(g, _):
            i, r = lax.div(g, ROWS // strip), pl.multiple_of(lax.rem(g, ROWS // strip) * strip, strip)
            here = pl.ds(pl.multiple_of(g * strip, strip), strip)
            t = own[parts * j + i, pl.ds(r, strip), :] + mem[_in_unit(s, j), here, :].astype(jnp.float32)
            if running:
                t = t + mem[_run_unit(s, j), here, :].astype(jnp.float32)
            if last:
                columns = pl.ds(pl.multiple_of(j * wide + i * SIDE, SIDE), SIDE)
                y_s[pl.ds(r, strip), columns] = (y_s[pl.ds(r, strip), columns].astype(jnp.float32) + t).astype(jnp.bfloat16)
            else:
                mem[_run_unit(s, j), here, :] = t.astype(jnp.bfloat16)

        lax.fori_loop(0, parts * ROWS // strip, some, None)

    def leave(j):
        columns = pl.ds(pl.multiple_of(j * wide, wide), wide)
        return pltpu.make_async_copy(y_s.at[:, columns], out_ref.at[:, columns], y_sem.at[j])

    def first(j, _):
        term(0, j).wait_recv()
        add(0, j, False, False)
        total(0, j).start()

    for which in range(2):
        finish(0, which)
    for j in range(SUBS):
        for load in wo_load(j):
            load.wait()
    pl.semaphore_wait(phase, 3)
    lax.fori_loop(0, SUBS, lambda j, _: terms(0, j), None)
    lax.fori_loop(0, SUBS, first, None)
    lax.fori_loop(0, 2, lambda i, _: attend(1, i), None)
    lax.fori_loop(0, SUBS, lambda j, _: terms(1, j), None)
    lax.fori_loop(0, 2, lambda i, _: attend(2, i), None)
    x_load.wait()

    def scatter(t, _):
        s, j = lax.div(t, SUBS), lax.rem(t, SUBS)
        total(s - 1, j).wait_recv()
        term(s, j).wait_recv()

        @pl.when(s < CHIPS - 1)
        def _():
            add(s, j, True, False)
            total(s, j).start()
            term(s - 1, j).wait_send()
            terms(s + 1, j)

        @pl.when(s == CHIPS - 1)
        def _():
            add(s, j, True, True)
            leave(j).start()

        @pl.when((s < CHIPS - 2) & (j < 2))
        def _():
            attend(s + 2, j)

    lax.fori_loop(SUBS, CHIPS * SUBS, scatter, None)

    def done(s, _):
        for j in range(SUBS):
            total(s, j).wait_send()

    lax.fori_loop(0, CHIPS - 1, done, None)
    for s in (CHIPS - 2, CHIPS - 1):
        for j in range(SUBS):
            term(s, j).wait_send()
    for j in range(SUBS):
        leave(j).wait()


def solution(mesh):
    def step(x, gain, wq, wk, wv, wo):
        depth, cols = wq.shape
        heads, tokens = cols // HEAD, 2 * CHIPS * ROWS
        here, there = pl.BlockSpec(memory_space=pltpu.VMEM), pl.BlockSpec(memory_space=pl.ANY)
        low = jnp.bfloat16
        return pl.pallas_call(
            _kernel,
            out_shape=jax.ShapeDtypeStruct((ROWS, depth), low),
            in_specs=[there] + [here] * 5 + [there] * 4,
            out_specs=there,
            scratch_shapes=[
                pltpu.VMEM((UNITS, SIDE, SIDE), low),
                pltpu.VMEM((ROWS, depth), low),
                pltpu.VMEM((heads, tokens, HEAD), low),
                pltpu.VMEM((heads, tokens, HEAD), low),
                pltpu.VMEM((heads, HEAD, tokens), low),
                pltpu.VMEM((depth // SIDE, ROWS, SIDE), jnp.float32),
                pltpu.VMEM((2, 2, ROWS, cols), low),
                pltpu.VMEM((2, heads, 1, ROWS), jnp.float32),
                pltpu.VMEM((2, heads, 1, ROWS), jnp.float32),
                pltpu.VMEM((2, heads, HEAD, ROWS), jnp.float32),
                *[pltpu.SemaphoreType.DMA((CHIPS - 1, SUBS))] * 2,
                *[pltpu.SemaphoreType.DMA((CHIPS, SUBS))] * 2,
                *[pltpu.SemaphoreType.DMA((CHIPS - 1, SUBS))] * 2,
                *[pltpu.SemaphoreType.DMA((CHIPS, SUBS))] * 2,
                pltpu.SemaphoreType.DMA,
                pltpu.SemaphoreType.DMA((SUBS,)),
                pltpu.SemaphoreType.DMA((3, SUBS)),
                pltpu.SemaphoreType.DMA((SUBS, depth // SUBS // SIDE)),
                pltpu.SemaphoreType.REGULAR,
                pltpu.SemaphoreType.REGULAR,
            ],
            compiler_params=pltpu.CompilerParams(collective_id=0, has_side_effects=True, vmem_limit_bytes=VMEM),
            cost_estimate=pl.CostEstimate(flops=8 * tokens * depth * cols, bytes_accessed=8 * depth * cols,
                                          transcendentals=heads * tokens * tokens // 2),
            name="attention_half",
        )(x, gain, *_tables(), *[w.reshape(-1, SIDE, cols) for w in (wq, wk, wv)], wo)

    tokens, columns = P(("dp", "tp"), None), P(None, "tp")
    return jax.shard_map(
        step,
        mesh=mesh,
        in_specs=(tokens, P(None), columns, columns, columns, P("tp", None)),
        out_specs=tokens,
        check_vma=False,
    )
```

```python
import functools

import jax
import jax.numpy as jnp
import numpy as np
from jax import lax
from jax.experimental import pallas as pl
from jax.experimental.pallas import tpu as pltpu
from jax.sharding import PartitionSpec as P

HEAD = 128
THETA = 10000
NEG = -1e30
HIDDEN = 2 * NEG
LOG2E = 1.4426950408889634
CHIPS = 8
ROWS = 128
SUBS = 4
SIDE = 512
KEYS = 256
VMEM = 67043328
MESH = pl.DeviceIdType.MESH


def _dot(a, b, ca=1, cb=0):
    return lax.dot_general(a, b, (((ca,), (cb,)), ((), ())), preferred_element_type=jnp.float32)


def _chip(pos):
    return pos + lax.div(pos, 4) * (11 - 2 * pos)


def _where():
    me = lax.axis_index("tp")
    core, chip = lax.rem(me, 2), lax.div(me, 2)
    pos = _chip(chip)
    after = 2 * _chip(lax.rem(pos + 1 + 6 * core, CHIPS)) + core
    before = 2 * _chip(lax.rem(pos + 7 - 6 * core, CHIPS)) + core
    return core, pos, after, before, me + 1 - 2 * core


def _owner(pos, steps, parity):
    return 2 * _chip(lax.rem(pos + steps * (7 - 6 * parity), CHIPS)) + parity


def _meet(devices):
    barrier = pltpu.get_barrier_semaphore()
    for device in devices:
        pl.semaphore_signal(barrier, inc=1, device_id={"tp": device}, device_id_type=MESH)
    return lambda: pl.semaphore_wait(barrier, len(devices))


def _send(src, dst, send_sem, recv_sem, device):
    return pltpu.make_async_remote_copy(src_ref=src, dst_ref=dst, send_sem=send_sem, recv_sem=recv_sem, device_id={"tp": device},
                                        device_id_type=MESH)


def _tables():
    rate = np.tile(float(THETA) ** (-np.arange(HEAD // 2) / (HEAD // 2)), 2)
    sign = np.where(np.arange(HEAD) < HEAD // 2, -1.0, 1.0)
    fine, coarse = np.arange(ROWS)[:, None] * rate, (np.arange(2 * CHIPS) * ROWS)[:, None, None] * rate
    return [jnp.asarray(t, jnp.float32) for t in (np.cos(fine), np.sin(fine) * sign, np.cos(coarse), np.sin(coarse) * sign)]


def _x_unit(s, j):
    return SUBS * s + j


def _x_pair(s, j):
    return 32 + SUBS * lax.rem(s, 4) + j


def _w_unit(p, k):
    return 48 + 16 * p + k


def _wo_unit(n):
    return n


def _run_unit(s, j):
    return 16 + SUBS * s + j


def _in_unit(s, j):
    return 48 + SUBS * s + j


def _out_unit(s, j):
    return 80 + SUBS * lax.rem(s, 2) + j


UNITS = 96


def _kernel(x_ref, gain_ref, cos_f, sin_f, cos_c, sin_c, wq_ref, wk_ref, wv_ref, wo_ref, out_ref,
            mem, y_s, q_s, k_s, v_s, own, seen, top_s, sum_s, mix_s,
            ring_send, ring_recv, pair_send, pair_recv, sum_send, sum_recv, term_send, term_recv, x_sem, y_sem, w_sem, wo_sem, credit, pair_phase, ring_phase):
    core, pos, after, before, partner = _where()
    depth = y_s.shape[1]
    heads = q_s.shape[0]
    wide = depth // SUBS
    parts = wide // SIDE
    met = _meet((after, before, partner))
    x_load = pltpu.make_async_copy(x_ref, y_s, x_sem)
    x_load.start()
    weights = (wq_ref, wk_ref, wv_ref)

    def w_load(p, j):
        return pltpu.make_async_copy(weights[p].at[pl.ds(parts * j, parts)], mem.at[pl.ds(_w_unit(p, parts * j), parts)], w_sem.at[p, j])

    def ring(s, j):
        return _send(mem.at[_x_unit(s, j)], mem.at[_x_unit(s + 1, j)], ring_send.at[s, j], ring_recv.at[s, j], after)

    def ring_two(s, j):
        return _send(mem.at[pl.ds(_x_unit(s, j), 2)], mem.at[pl.ds(_x_unit(s + 1, j), 2)], ring_send.at[s, j], ring_recv.at[s, j], after)

    def pair(s, j):
        return _send(mem.at[_x_unit(s, j)], mem.at[_x_pair(s, j)], pair_send.at[s, j], pair_recv.at[s, j], partner)

    e = HEAD**-0.5 * LOG2E

    def attend_keys(which, device, starts, size, masked):
        here = pl.ds(pl.multiple_of(device * ROWS, ROWS), ROWS)
        keys = [pl.ds(pl.multiple_of(start, size), size) for start in starts]
        scores = [_dot(jnp.concatenate([k_s[h, part, :] for part in keys], axis=0), q_s[h, here, :], 1, 1) for h in range(heads)]
        if masked:
            gap = lax.broadcasted_iota(jnp.int32, (size, ROWS), 1) - lax.broadcasted_iota(jnp.int32, (size, ROWS), 0)
            ok = jnp.concatenate([gap - start for start in starts], axis=0) >= -device * ROWS
            scores = [jnp.where(ok, t, HIDDEN) for t in scores]
        weights = []
        for h, t in enumerate(scores):
            old = top_s[which, h]
            top = jnp.maximum(old, t.max(axis=0, keepdims=True))
            p = jnp.exp2((t - top) * e)
            keep = jnp.exp2((old - top) * e)
            top_s[which, h] = top
            sum_s[which, h] = sum_s[which, h] * keep + p.sum(axis=0, keepdims=True)
            weights.append((p.astype(jnp.bfloat16), keep))
        for h, (p, keep) in enumerate(weights):
            mix_s[which, h] = mix_s[which, h] * keep + _dot(jnp.concatenate([v_s[h, :, part] for part in keys], axis=1), p)

    def begin(which):
        top_s[which] = jnp.full(top_s.shape[1:], NEG, jnp.float32)
        sum_s[which] = jnp.zeros(sum_s.shape[1:], jnp.float32)
        mix_s[which] = jnp.zeros(mix_s.shape[1:], jnp.float32)

    def finish(s, which):
        for h in range(heads):
            out = (mix_s[which, h] * (1 / sum_s[which, h])).T
            seen[lax.rem(s, 2), which, :, h * HEAD : (h + 1) * HEAD] = out.astype(jnp.bfloat16)

    def block_of(s, which):
        return _owner(pos, s + 1, lax.rem(core + which, 2))

    def attend(s, which):
        device = block_of(s, which)
        begin(which)
        whole = lax.div(device * ROWS, KEYS)
        lax.fori_loop(0, whole, lambda i, _: attend_keys(which, device, [i * KEYS], KEYS, False), None)
        attend_keys(which, device, [whole * KEYS], KEYS, True)
        finish(s, which)

    def ahead(s):
        starts = [_owner(pos, s, parity) * ROWS for parity in range(2)]
        for which in range(2):
            attend_keys(which, block_of(0, which), starts, ROWS, True)

    for n in range(6):
        own[n] = jnp.zeros_like(own[n])
    for which in range(2):
        begin(which)
    x_load.wait()
    for j in range(SUBS):
        for p in range(3):
            w_load(p, j).start()
    group = 16
    scales = []
    for r in range(0, ROWS, group):
        wide_x = y_s[r : r + group, :].astype(jnp.float32)
        scales.append(lax.rsqrt(jnp.sum(wide_x * wide_x, -1, keepdims=True) * (1 / depth) + 1e-6))
    for j in range(SUBS):
        for i in range(parts):
            here = slice(j * wide + i * SIDE, j * wide + (i + 1) * SIDE)
            gain = gain_ref[here].astype(jnp.float32).reshape(1, SIDE)
            for r in range(0, ROWS, group):
                t = y_s[r : r + group, here].astype(jnp.float32) * scales[r // group] * gain
                mem[_x_unit(0, j), i * ROWS + r : i * ROWS + r + group, :] = t.astype(jnp.bfloat16)
        if j == 0:
            met()
        ring(0, j).start()
        pair(0, j).start()

    def project(t):
        s, j = lax.div(t, SUBS), lax.rem(t, SUBS)
        pair(s, j).wait_recv()
        mine, theirs = _x_unit(s, j), _x_pair(s, j)
        units = mine + core * (theirs - mine), theirs + core * (mine - theirs)
        a = [jnp.concatenate([mem[u, i * ROWS : (i + 1) * ROWS, :] for i in range(parts)], axis=1) for u in units]
        a = jnp.concatenate(a, axis=0)
        for p in range(3):
            @pl.when(s == 0)
            def _():
                w_load(p, j).wait()

            part = _dot(a, mem[pl.ds(_w_unit(p, parts * j), parts)].reshape(wide, SIDE))
            own[p] += part[:ROWS]
            own[3 + p] += part[ROWS:]

        @pl.when(j == SUBS - 1)
        def _():
            for parity in range(2):
                device = _owner(pos, s, parity)
                here = pl.ds(pl.multiple_of(device * ROWS, ROWS), ROWS)
                cf, sf, cc, sc = cos_f[...], sin_f[...], cos_c[device], sin_c[device]
                cos, sin = cc * cf - sc * sf, sc * cf + cc * sf
                for p in range(3):
                    for h in range(heads):
                        t = own[3 * parity + p, :, h * HEAD : (h + 1) * HEAD].astype(jnp.bfloat16).astype(jnp.float32)
                        if p < 2:
                            (q_s, k_s)[p][h, here, :] = (t * cos + pltpu.roll(t, HEAD // 2, 1) * sin).astype(jnp.bfloat16)
                        else:
                            v_s[h, :, here] = t.T.astype(jnp.bfloat16)
            for n in range(6):
                own[n] = jnp.zeros_like(own[n])

            @pl.when(s < 4)
            def _():
                pl.semaphore_signal(credit, inc=1, device_id={"tp": partner}, device_id_type=MESH)

            @pl.when(s == 1)
            def _():
                ahead(0)

            @pl.when(s >= 1)
            def _():
                ahead(s)

    def wo_load(j):
        return [pltpu.make_async_copy(wo_ref.at[:, pl.ds((parts * j + i) * SIDE, SIDE)], mem.at[_wo_unit(parts * j + i)], wo_sem.at[j, i])
                for i in range(parts)]

    def arrive(s, j, one, two):
        @pl.when((s == 1) | (s == CHIPS - 1))
        def _():
            one(s - 1, j).wait_recv()

        @pl.when((s > 1) & (s < CHIPS - 1) & (lax.rem(j, 2) == 0))
        def _():
            two(s - 1, j).wait_recv()

    def depart(s, one, two):
        @pl.when((s == 0) | (s == CHIPS - 2))
        def _():
            for j in range(SUBS):
                one(s, j).wait_send()

        @pl.when((s > 0) & (s < CHIPS - 2))
        def _():
            for j in range(0, SUBS, 2):
                two(s, j).wait_send()

    def gather(t, _):
        @pl.when((t >= SUBS) & (t < CHIPS * SUBS))
        def _():
            s, j = lax.div(t, SUBS), lax.rem(t, SUBS)
            arrive(s, j, ring, ring_two)

            @pl.when(s == CHIPS - 2)
            def _():
                ring(s, j).start()

            @pl.when((s == 1) & (lax.rem(j, 2) == 1))
            def _():
                ring_two(s, j - 1).start()

            @pl.when((s > 1) & (s < CHIPS - 2) & (lax.rem(j, 2) == 0))
            def _():
                ring_two(s, j).start()

            @pl.when((s >= 4) & (j == 0))
            def _():
                pl.semaphore_wait(credit, 1)

            pair(s, j).start()

        project(t - 1)

        @pl.when(t == 6 * SUBS)
        def _():
            def sent(s, _):
                depart(s, ring, ring_two)
                for j in range(SUBS):
                    pair(s, j).wait_send()

            lax.fori_loop(0, 4, sent, None)
            for j in range(SUBS):
                for load in wo_load(j):
                    load.start()

    lax.fori_loop(1, CHIPS * SUBS + 1, gather, None)

    def sent(s, _):
        depart(s, ring, ring_two)
        for j in range(SUBS):
            pair(s, j).wait_send()

    lax.fori_loop(4, CHIPS, sent, None)
    for semaphore, device in ((pair_phase, partner), (ring_phase, before)):
        pl.semaphore_signal(semaphore, inc=1, device_id={"tp": device}, device_id_type=MESH)
    x_load.start()
    def total(s, j):
        return _send(mem.at[_run_unit(s, j)], mem.at[_run_unit(s + 1, j)], sum_send.at[s, j], sum_recv.at[s, j], after)

    def total_two(s, j):
        return _send(mem.at[pl.ds(_run_unit(s, j), 2)], mem.at[pl.ds(_run_unit(s + 1, j), 2)], sum_send.at[s, j], sum_recv.at[s, j], after)

    def term(s, j):
        return _send(mem.at[_out_unit(s, j)], mem.at[_in_unit(s, j)], term_send.at[s, j], term_recv.at[s, j], partner)

    def terms(s, j):
        both = seen[lax.rem(s, 2)].reshape(2 * ROWS, heads * HEAD)
        for i in range(parts):
            t = _dot(both, mem[_wo_unit(parts * j + i)])
            own[parts * j + i] = t[:ROWS]
            mem[_out_unit(s, j), i * ROWS : (i + 1) * ROWS, :] = t[ROWS:].astype(jnp.bfloat16)
        term(s, j).start()

    strip = 64

    def add(s, j, running, last):
        def some(g, _):
            i, r = lax.div(g, ROWS // strip), pl.multiple_of(lax.rem(g, ROWS // strip) * strip, strip)
            here = pl.ds(pl.multiple_of(g * strip, strip), strip)
            t = own[parts * j + i, pl.ds(r, strip), :] + mem[_in_unit(s, j), here, :].astype(jnp.float32)
            if running:
                t = t + mem[_run_unit(s, j), here, :].astype(jnp.float32)
            if last:
                columns = pl.ds(pl.multiple_of(j * wide + i * SIDE, SIDE), SIDE)
                y_s[pl.ds(r, strip), columns] = (y_s[pl.ds(r, strip), columns].astype(jnp.float32) + t).astype(jnp.bfloat16)
            else:
                mem[_run_unit(s, j), here, :] = t.astype(jnp.bfloat16)

        lax.fori_loop(0, parts * ROWS // strip, some, None)

    def leave(j):
        columns = pl.ds(pl.multiple_of(j * wide, wide), wide)
        return pltpu.make_async_copy(y_s.at[:, columns], out_ref.at[:, columns], y_sem.at[j])

    def first(j, _):
        term(0, j).wait_recv()
        add(0, j, False, False)
        total(0, j).start()

    for which in range(2):
        finish(0, which)
    for j in range(SUBS):
        for load in wo_load(j):
            load.wait()
    pl.semaphore_wait(pair_phase, 1)
    lax.fori_loop(0, SUBS, lambda j, _: terms(0, j), None)
    pl.semaphore_wait(ring_phase, 1)
    lax.fori_loop(0, SUBS, first, None)
    lax.fori_loop(0, 2, lambda i, _: attend(1, i), None)
    lax.fori_loop(0, SUBS, lambda j, _: terms(1, j), None)
    lax.fori_loop(0, 2, lambda i, _: attend(2, i), None)
    x_load.wait()

    def scatter(t, _):
        s, j = lax.div(t, SUBS), lax.rem(t, SUBS)
        arrive(s, j, total, total_two)
        term(s, j).wait_recv()

        @pl.when(s < CHIPS - 1)
        def _():
            add(s, j, True, False)

            @pl.when(s == CHIPS - 2)
            def _():
                total(s, j).start()

            @pl.when((s < CHIPS - 2) & (lax.rem(j, 2) == 1))
            def _():
                total_two(s, j - 1).start()

            term(s - 1, j).wait_send()
            terms(s + 1, j)

        @pl.when(s == CHIPS - 1)
        def _():
            add(s, j, True, True)
            leave(j).start()

        @pl.when((s < CHIPS - 2) & (j < 2))
        def _():
            attend(s + 2, j)

    lax.fori_loop(SUBS, CHIPS * SUBS, scatter, None)

    def done(s, _):
        depart(s, total, total_two)

    lax.fori_loop(0, CHIPS - 1, done, None)
    for s in (CHIPS - 2, CHIPS - 1):
        for j in range(SUBS):
            term(s, j).wait_send()
    for j in range(SUBS):
        leave(j).wait()


def solution(mesh):
    def step(x, gain, wq, wk, wv, wo):
        depth, cols = wq.shape
        heads, tokens = cols // HEAD, 2 * CHIPS * ROWS
        here, there = pl.BlockSpec(memory_space=pltpu.VMEM), pl.BlockSpec(memory_space=pl.ANY)
        low = jnp.bfloat16
        return pl.pallas_call(
            _kernel,
            out_shape=jax.ShapeDtypeStruct((ROWS, depth), low),
            in_specs=[there] + [here] * 5 + [there] * 4,
            out_specs=there,
            scratch_shapes=[
                pltpu.VMEM((UNITS, SIDE, SIDE), low),
                pltpu.VMEM((ROWS, depth), low),
                pltpu.VMEM((heads, tokens, HEAD), low),
                pltpu.VMEM((heads, tokens, HEAD), low),
                pltpu.VMEM((heads, HEAD, tokens), low),
                pltpu.VMEM((depth // SIDE, ROWS, SIDE), jnp.float32),
                pltpu.VMEM((2, 2, ROWS, cols), low),
                pltpu.VMEM((2, heads, 1, ROWS), jnp.float32),
                pltpu.VMEM((2, heads, 1, ROWS), jnp.float32),
                pltpu.VMEM((2, heads, HEAD, ROWS), jnp.float32),
                *[pltpu.SemaphoreType.DMA((CHIPS - 1, SUBS))] * 2,
                *[pltpu.SemaphoreType.DMA((CHIPS, SUBS))] * 2,
                *[pltpu.SemaphoreType.DMA((CHIPS - 1, SUBS))] * 2,
                *[pltpu.SemaphoreType.DMA((CHIPS, SUBS))] * 2,
                pltpu.SemaphoreType.DMA,
                pltpu.SemaphoreType.DMA((SUBS,)),
                pltpu.SemaphoreType.DMA((3, SUBS)),
                pltpu.SemaphoreType.DMA((SUBS, depth // SUBS // SIDE)),
                *[pltpu.SemaphoreType.REGULAR] * 3,
            ],
            compiler_params=pltpu.CompilerParams(collective_id=0, has_side_effects=True, vmem_limit_bytes=VMEM),
            cost_estimate=pl.CostEstimate(flops=8 * tokens * depth * cols, bytes_accessed=8 * depth * cols,
                                          transcendentals=heads * tokens * tokens // 2),
            name="attention_half",
        )(x, gain, *_tables(), *[w.reshape(-1, SIDE, cols) for w in (wq, wk, wv)], wo)

    tokens, columns = P(("dp", "tp"), None), P(None, "tp")
    return jax.shard_map(
        step,
        mesh=mesh,
        in_specs=(tokens, P(None), columns, columns, columns, P("tp", None)),
        out_specs=tokens,
        check_vma=False,
    )
```

```python
import functools

import jax
import jax.numpy as jnp
import numpy as np
from jax import lax
from jax.experimental import pallas as pl
from jax.experimental.pallas import tpu as pltpu
from jax.sharding import PartitionSpec as P

HEAD = 128
THETA = 10000
NEG = -1e30
HIDDEN = 2 * NEG
LOG2E = 1.4426950408889634
CHIPS = 8
ROWS = 128
SUBS = 8
HALF = SUBS // 2
SIDE = 512
TALL = 256
KEYS = 256
VMEM = 67043328
MESH = pl.DeviceIdType.MESH


def _dot(a, b, ca=1, cb=0):
    return lax.dot_general(a, b, (((ca,), (cb,)), ((), ())), preferred_element_type=jnp.float32)


def _chip(pos):
    return pos + lax.div(pos, 4) * (11 - 2 * pos)


def _where():
    me = lax.axis_index("tp")
    core, chip = lax.rem(me, 2), lax.div(me, 2)
    pos = _chip(chip)
    after = 2 * _chip(lax.rem(pos + 1 + 6 * core, CHIPS)) + core
    before = 2 * _chip(lax.rem(pos + 7 - 6 * core, CHIPS)) + core
    return core, pos, after, before, me + 1 - 2 * core


def _owner(pos, steps, parity):
    return 2 * _chip(lax.rem(pos + steps * (7 - 6 * parity), CHIPS)) + parity


def _meet(devices):
    barrier = pltpu.get_barrier_semaphore()
    for device in devices:
        pl.semaphore_signal(barrier, inc=1, device_id={"tp": device}, device_id_type=MESH)
    return lambda: pl.semaphore_wait(barrier, len(devices))


def _send(src, dst, send_sem, recv_sem, device):
    return pltpu.make_async_remote_copy(src_ref=src, dst_ref=dst, send_sem=send_sem, recv_sem=recv_sem, device_id={"tp": device},
                                        device_id_type=MESH)


def _tables():
    rate = np.tile(float(THETA) ** (-np.arange(HEAD // 2) / (HEAD // 2)), 2)
    sign = np.where(np.arange(HEAD) < HEAD // 2, -1.0, 1.0)
    fine, coarse = np.arange(ROWS)[:, None] * rate, (np.arange(2 * CHIPS) * ROWS)[:, None, None] * rate
    return [jnp.asarray(t, jnp.float32) for t in (np.cos(fine), np.sin(fine) * sign, np.cos(coarse), np.sin(coarse) * sign)]


def _x_unit(s, j):
    return SUBS * s + j


def _x_pair(s, j):
    return 64 + SUBS * lax.rem(s, 4) + j


def _w_unit(p, k):
    return 96 + 32 * p + k


def _wo_unit(n):
    return 2 * n


def _run_unit(s, j):
    return 32 + SUBS * s + j


def _in_unit(s, j):
    return 96 + SUBS * s + j


def _out_unit(s, j):
    return 160 + SUBS * lax.rem(s, 2) + j


UNITS = 192


def _kernel(x_ref, gain_ref, cos_f, sin_f, cos_c, sin_c, wq_ref, wk_ref, wv_ref, wo_ref, out_ref,
            mem, y_s, q_s, k_s, v_s, own, seen, top_s, sum_s, mix_s,
            ring_send, ring_recv, pair_send, pair_recv, sum_send, sum_recv, term_send, term_recv, x_sem, y_sem, w_sem, wo_sem, credit, pair_phase, ring_phase):
    core, pos, after, before, partner = _where()
    depth = y_s.shape[1]
    heads = q_s.shape[0]
    wide = depth // SUBS
    parts = wide // SIDE
    deep = wide // TALL
    met = _meet((after, before, partner))
    x_loads = []
    for n, here in enumerate(pl.ds(r, ROWS // 4) for r in range(0, ROWS, ROWS // 4)):
        x_loads.append(pltpu.make_async_copy(x_ref.at[here], y_s.at[here], x_sem.at[n]))
    for load in x_loads:
        load.start()
    weights = (wq_ref, wk_ref, wv_ref)

    def w_load(p, j):
        return pltpu.make_async_copy(weights[p].at[pl.ds(deep * j, deep)], mem.at[pl.ds(_w_unit(p, deep * j), deep)], w_sem.at[p, j])

    def ring(s, j):
        return _send(mem.at[_x_unit(s, j)], mem.at[_x_unit(s + 1, j)], ring_send.at[s, j], ring_recv.at[s, j], after)

    def ring_half(s, j):
        return _send(mem.at[pl.ds(_x_unit(s, j), HALF)], mem.at[pl.ds(_x_unit(s + 1, j), HALF)], ring_send.at[s, j], ring_recv.at[s, j], after)

    def pair(s, j):
        return _send(mem.at[_x_unit(s, j)], mem.at[_x_pair(s, j)], pair_send.at[s, j], pair_recv.at[s, j], partner)

    e = HEAD**-0.5 * LOG2E

    def attend_keys(which, device, starts, size, masked):
        here = pl.ds(pl.multiple_of(device * ROWS, ROWS), ROWS)
        keys = [pl.ds(pl.multiple_of(start, size), size) for start in starts]
        scores = [_dot(jnp.concatenate([k_s[h, part, :] for part in keys], axis=0), q_s[h, here, :], 1, 1) for h in range(heads)]
        if masked:
            gap = lax.broadcasted_iota(jnp.int32, (size, ROWS), 1) - lax.broadcasted_iota(jnp.int32, (size, ROWS), 0)
            ok = jnp.concatenate([gap - start for start in starts], axis=0) >= -device * ROWS
            scores = [jnp.where(ok, t, HIDDEN) for t in scores]
        weights = []
        for h, t in enumerate(scores):
            old = top_s[which, h]
            top = jnp.maximum(old, t.max(axis=0, keepdims=True))
            p = jnp.exp2((t - top) * e)
            keep = jnp.exp2((old - top) * e)
            top_s[which, h] = top
            sum_s[which, h] = sum_s[which, h] * keep + p.sum(axis=0, keepdims=True)
            weights.append((p.astype(jnp.bfloat16), keep))
        for h, (p, keep) in enumerate(weights):
            mix_s[which, h] = mix_s[which, h] * keep + _dot(jnp.concatenate([v_s[h, :, part] for part in keys], axis=1), p)

    def begin(which):
        top_s[which] = jnp.full(top_s.shape[1:], NEG, jnp.float32)
        sum_s[which] = jnp.zeros(sum_s.shape[1:], jnp.float32)
        mix_s[which] = jnp.zeros(mix_s.shape[1:], jnp.float32)

    def finish(s, which):
        for h in range(heads):
            out = (mix_s[which, h] * (1 / sum_s[which, h])).T
            seen[lax.rem(s, 2), which, :, h * HEAD : (h + 1) * HEAD] = out.astype(jnp.bfloat16)

    def block_of(s, which):
        return _owner(pos, s + 1, lax.rem(core + which, 2))

    def attend(s, which):
        device = block_of(s, which)
        begin(which)
        whole = lax.div(device * ROWS, KEYS)
        lax.fori_loop(0, whole, lambda i, _: attend_keys(which, device, [i * KEYS], KEYS, False), None)
        attend_keys(which, device, [whole * KEYS], KEYS, True)
        finish(s, which)

    def ahead(s):
        starts = [_owner(pos, s, parity) * ROWS for parity in range(2)]
        for which in range(2):
            attend_keys(which, block_of(0, which), starts, ROWS, True)

    for n in range(6):
        own[n] = jnp.zeros_like(own[n])
    for which in range(2):
        begin(which)
    group = 16
    scales = []
    for r in range(0, ROWS, group):
        if r % (ROWS // 4) == 0:
            x_loads[r // (ROWS // 4)].wait()
        wide_x = y_s[r : r + group, :].astype(jnp.float32)
        scales.append(lax.rsqrt(jnp.sum(wide_x * wide_x, -1, keepdims=True) * (1 / depth) + 1e-6))
    for j in range(SUBS):
        for p in range(3):
            w_load(p, j).start()
    for j in range(SUBS):
        for i in range(parts):
            here = slice(j * wide + i * SIDE, j * wide + (i + 1) * SIDE)
            gain = gain_ref[here].astype(jnp.float32).reshape(1, SIDE)
            for r in range(0, ROWS, group):
                t = y_s[r : r + group, here].astype(jnp.float32) * scales[r // group] * gain
                mem[_x_unit(0, j), i * ROWS + r : i * ROWS + r + group, :] = t.astype(jnp.bfloat16)
        if j == 0:
            met()
        ring(0, j).start()
        pair(0, j).start()

    def project(t):
        s, j = lax.div(t, SUBS), lax.rem(t, SUBS)
        pair(s, j).wait_recv()
        mine, theirs = _x_unit(s, j), _x_pair(s, j)
        units = mine + core * (theirs - mine), theirs + core * (mine - theirs)
        a = [jnp.concatenate([mem[u, i * ROWS : (i + 1) * ROWS, :] for i in range(parts)], axis=1) for u in units]
        a = jnp.concatenate(a, axis=0)
        for p in range(3):
            @pl.when(s == 0)
            def _():
                w_load(p, j).wait()

            part = _dot(a, mem[pl.ds(_w_unit(p, deep * j), deep)].reshape(wide, SIDE))
            own[p] += part[:ROWS]
            own[3 + p] += part[ROWS:]

        @pl.when(j == SUBS - 1)
        def _():
            for parity in range(2):
                device = _owner(pos, s, parity)
                here = pl.ds(pl.multiple_of(device * ROWS, ROWS), ROWS)
                cf, sf, cc, sc = cos_f[...], sin_f[...], cos_c[device], sin_c[device]
                cos, sin = cc * cf - sc * sf, sc * cf + cc * sf
                for p in range(3):
                    for h in range(heads):
                        t = own[3 * parity + p, :, h * HEAD : (h + 1) * HEAD].astype(jnp.bfloat16).astype(jnp.float32)
                        if p < 2:
                            (q_s, k_s)[p][h, here, :] = (t * cos + pltpu.roll(t, HEAD // 2, 1) * sin).astype(jnp.bfloat16)
                        else:
                            v_s[h, :, here] = t.T.astype(jnp.bfloat16)
            for n in range(6):
                own[n] = jnp.zeros_like(own[n])

            @pl.when(s < 4)
            def _():
                pl.semaphore_signal(credit, inc=1, device_id={"tp": partner}, device_id_type=MESH)

            @pl.when(s == 1)
            def _():
                ahead(0)

            @pl.when(s >= 1)
            def _():
                ahead(s)

    def wo_load(j):
        return [pltpu.make_async_copy(wo_ref.at[:, :, pl.ds((parts * j + i) * SIDE, SIDE)], mem.at[pl.ds(_wo_unit(parts * j + i), 2)], wo_sem.at[j, i])
                for i in range(parts)]

    def arrive(s, j, one, half):
        @pl.when((s == 1) | (s == CHIPS - 1))
        def _():
            one(s - 1, j).wait_recv()

        @pl.when((s > 1) & (s < CHIPS - 1) & (lax.rem(j, HALF) == 0))
        def _():
            half(s - 1, j).wait_recv()

    def depart(s, one, half):
        @pl.when((s == 0) | (s == CHIPS - 2))
        def _():
            for j in range(SUBS):
                one(s, j).wait_send()

        @pl.when((s > 0) & (s < CHIPS - 2))
        def _():
            for j in range(0, SUBS, HALF):
                half(s, j).wait_send()

    def gather(t, _):
        @pl.when((t >= SUBS) & (t < CHIPS * SUBS))
        def _():
            s, j = lax.div(t, SUBS), lax.rem(t, SUBS)
            arrive(s, j, ring, ring_half)

            @pl.when(s == CHIPS - 2)
            def _():
                ring(s, j).start()

            @pl.when((s == 1) & (lax.rem(j, HALF) == HALF - 1))
            def _():
                ring_half(s, j - HALF + 1).start()

            @pl.when((s > 1) & (s < CHIPS - 2) & (lax.rem(j, HALF) == 0))
            def _():
                ring_half(s, j).start()

            @pl.when((s >= 4) & (j == 0))
            def _():
                pl.semaphore_wait(credit, 1)

            pair(s, j).start()

        project(t - 1)

        def sent(s, _):
            depart(s, ring, ring_half)
            for j in range(SUBS):
                pair(s, j).wait_send()

        @pl.when(t == 6 * SUBS)
        def _():
            lax.fori_loop(0, 4, sent, None)
            for j in range(SUBS):
                for load in wo_load(j):
                    load.start()

        @pl.when(t == 7 * SUBS)
        def _():
            lax.fori_loop(4, 6, sent, None)
            for j in range(SUBS):
                pair(6, j).wait_send()

        @pl.when(t > 7 * SUBS)
        def _():
            j = t - 1 - 7 * SUBS
            ring(6, j).wait_send()
            pair(7, j).wait_send()

    lax.fori_loop(1, CHIPS * SUBS + 1, gather, None)
    for semaphore, device in ((pair_phase, partner), (ring_phase, before)):
        pl.semaphore_signal(semaphore, inc=1, device_id={"tp": device}, device_id_type=MESH)
    for load in x_loads:
        load.start()
    def total(s, j):
        return _send(mem.at[_run_unit(s, j)], mem.at[_run_unit(s + 1, j)], sum_send.at[s, j], sum_recv.at[s, j], after)

    def total_half(s, j):
        return _send(mem.at[pl.ds(_run_unit(s, j), HALF)], mem.at[pl.ds(_run_unit(s + 1, j), HALF)], sum_send.at[s, j], sum_recv.at[s, j], after)

    def term(s, j):
        return _send(mem.at[_out_unit(s, j)], mem.at[_in_unit(s, j)], term_send.at[s, j], term_recv.at[s, j], partner)

    def terms(s, j):
        both = seen[lax.rem(s, 2)].reshape(2 * ROWS, heads * HEAD)
        for i in range(parts):
            t = _dot(both, mem[pl.ds(_wo_unit(parts * j + i), 2)].reshape(heads * HEAD, SIDE))
            own[parts * j + i] = t[:ROWS]
            mem[_out_unit(s, j), i * ROWS : (i + 1) * ROWS, :] = t[ROWS:].astype(jnp.bfloat16)
        term(s, j).start()

    strip = 64

    def add(s, j, running, last):
        def some(g, _):
            i, r = lax.div(g, ROWS // strip), pl.multiple_of(lax.rem(g, ROWS // strip) * strip, strip)
            here = pl.ds(pl.multiple_of(g * strip, strip), strip)
            t = own[parts * j + i, pl.ds(r, strip), :] + mem[_in_unit(s, j), here, :].astype(jnp.float32)
            if running:
                t = t + mem[_run_unit(s, j), here, :].astype(jnp.float32)
            if last:
                columns = pl.ds(pl.multiple_of(j * wide + i * SIDE, SIDE), SIDE)
                y_s[pl.ds(r, strip), columns] = (y_s[pl.ds(r, strip), columns].astype(jnp.float32) + t).astype(jnp.bfloat16)
            else:
                mem[_run_unit(s, j), here, :] = t.astype(jnp.bfloat16)

        lax.fori_loop(0, parts * ROWS // strip, some, None)

    def leave(j):
        columns = pl.ds(pl.multiple_of(j * wide, wide), wide)
        return pltpu.make_async_copy(y_s.at[:, columns], out_ref.at[:, columns], y_sem.at[j])

    def first(j, _):
        term(0, j).wait_recv()
        add(0, j, False, False)
        total(0, j).start()

    for which in range(2):
        finish(0, which)
    for j in range(SUBS):
        for load in wo_load(j):
            load.wait()
    pl.semaphore_wait(pair_phase, 1)
    lax.fori_loop(0, SUBS, lambda j, _: terms(0, j), None)
    pl.semaphore_wait(ring_phase, 1)
    lax.fori_loop(0, SUBS, first, None)
    lax.fori_loop(0, 2, lambda i, _: attend(1, i), None)
    lax.fori_loop(0, SUBS, lambda j, _: terms(1, j), None)
    lax.fori_loop(0, 2, lambda i, _: attend(2, i), None)
    for load in x_loads:
        load.wait()

    def scatter(t, _):
        s, j = lax.div(t, SUBS), lax.rem(t, SUBS)
        arrive(s, j, total, total_half)
        term(s, j).wait_recv()

        @pl.when(s < CHIPS - 1)
        def _():
            add(s, j, True, False)

            @pl.when(s == CHIPS - 2)
            def _():
                total(s, j).start()

            @pl.when((s < CHIPS - 2) & (lax.rem(j, HALF) == HALF - 1))
            def _():
                total_half(s, j - HALF + 1).start()

            term(s - 1, j).wait_send()
            terms(s + 1, j)

        @pl.when(s == CHIPS - 1)
        def _():
            add(s, j, True, True)
            leave(j).start()
            total(s - 1, j).wait_send()
            term(s - 1, j).wait_send()
            term(s, j).wait_send()

        @pl.when(t == (CHIPS - 1) * SUBS - 1)
        def _():
            lax.fori_loop(0, CHIPS - 2, lambda s, _: depart(s, total, total_half), None)

        @pl.when((s < CHIPS - 2) & (lax.rem(j, HALF) == HALF - 1))
        def _():
            attend(s + 2, lax.div(j, HALF))

    lax.fori_loop(SUBS, CHIPS * SUBS, scatter, None)

    for j in range(SUBS):
        leave(j).wait()


def solution(mesh):
    def step(x, gain, wq, wk, wv, wo):
        depth, cols = wq.shape
        heads, tokens = cols // HEAD, 2 * CHIPS * ROWS
        here, there = pl.BlockSpec(memory_space=pltpu.VMEM), pl.BlockSpec(memory_space=pl.ANY)
        low = jnp.bfloat16
        return pl.pallas_call(
            _kernel,
            out_shape=jax.ShapeDtypeStruct((ROWS, depth), low),
            in_specs=[there] + [here] * 5 + [there] * 4,
            out_specs=there,
            scratch_shapes=[
                pltpu.VMEM((UNITS, TALL, SIDE), low),
                pltpu.VMEM((ROWS, depth), low),
                pltpu.VMEM((heads, tokens, HEAD), low),
                pltpu.VMEM((heads, tokens, HEAD), low),
                pltpu.VMEM((heads, HEAD, tokens), low),
                pltpu.VMEM((depth // SIDE, ROWS, SIDE), jnp.float32),
                pltpu.VMEM((2, 2, ROWS, cols), low),
                pltpu.VMEM((2, heads, 1, ROWS), jnp.float32),
                pltpu.VMEM((2, heads, 1, ROWS), jnp.float32),
                pltpu.VMEM((2, heads, HEAD, ROWS), jnp.float32),
                *[pltpu.SemaphoreType.DMA((CHIPS - 1, SUBS))] * 2,
                *[pltpu.SemaphoreType.DMA((CHIPS, SUBS))] * 2,
                *[pltpu.SemaphoreType.DMA((CHIPS - 1, SUBS))] * 2,
                *[pltpu.SemaphoreType.DMA((CHIPS, SUBS))] * 2,
                pltpu.SemaphoreType.DMA((4,)),
                pltpu.SemaphoreType.DMA((SUBS,)),
                pltpu.SemaphoreType.DMA((3, SUBS)),
                pltpu.SemaphoreType.DMA((SUBS, depth // SUBS // SIDE)),
                *[pltpu.SemaphoreType.REGULAR] * 3,
            ],
            compiler_params=pltpu.CompilerParams(collective_id=0, has_side_effects=True, vmem_limit_bytes=VMEM),
            cost_estimate=pl.CostEstimate(flops=8 * tokens * depth * cols, bytes_accessed=8 * depth * cols,
                                          transcendentals=heads * tokens * tokens // 2),
            name="attention_half",
        )(x, gain, *_tables(), *[w.reshape(-1, TALL, cols) for w in (wq, wk, wv)], wo.reshape(-1, TALL, depth))

    tokens, columns = P(("dp", "tp"), None), P(None, "tp")
    return jax.shard_map(
        step,
        mesh=mesh,
        in_specs=(tokens, P(None), columns, columns, columns, P("tp", None)),
        out_specs=tokens,
        check_vma=False,
    )
```

```python
import functools

import jax
import jax.numpy as jnp
import numpy as np
from jax import lax
from jax.experimental import pallas as pl
from jax.experimental.pallas import tpu as pltpu
from jax.sharding import PartitionSpec as P

HEAD = 128
THETA = 10000
NEG = -1e30
HIDDEN = 2 * NEG
LOG2E = 1.4426950408889634
CHIPS = 8
ROWS = 128
SUBS = 8
HALF = SUBS // 2
SIDE = 512
TALL = 256
KEYS = 256
VMEM = 67043328
MESH = pl.DeviceIdType.MESH


def _dot(a, b, ca=1, cb=0):
    return lax.dot_general(a, b, (((ca,), (cb,)), ((), ())), preferred_element_type=jnp.float32)


def _chip(pos):
    return pos + lax.div(pos, 4) * (11 - 2 * pos)


def _where():
    me = lax.axis_index("tp")
    core, chip = lax.rem(me, 2), lax.div(me, 2)
    pos = _chip(chip)
    after = 2 * _chip(lax.rem(pos + 1 + 6 * core, CHIPS)) + core
    before = 2 * _chip(lax.rem(pos + 7 - 6 * core, CHIPS)) + core
    return core, pos, after, before, me + 1 - 2 * core


def _owner(pos, steps, parity):
    return 2 * _chip(lax.rem(pos + steps * (7 - 6 * parity), CHIPS)) + parity


def _meet(devices):
    barrier = pltpu.get_barrier_semaphore()
    for device in devices:
        pl.semaphore_signal(barrier, inc=1, device_id={"tp": device}, device_id_type=MESH)
    return lambda: pl.semaphore_wait(barrier, len(devices))


def _send(src, dst, send_sem, recv_sem, device):
    return pltpu.make_async_remote_copy(src_ref=src, dst_ref=dst, send_sem=send_sem, recv_sem=recv_sem, device_id={"tp": device},
                                        device_id_type=MESH)


def _tables():
    rate = np.tile(float(THETA) ** (-np.arange(HEAD // 2) / (HEAD // 2)), 2)
    sign = np.where(np.arange(HEAD) < HEAD // 2, -1.0, 1.0)
    fine, coarse = np.arange(ROWS)[:, None] * rate, (np.arange(2 * CHIPS) * ROWS)[:, None, None] * rate
    return [jnp.asarray(t, jnp.float32) for t in (np.cos(fine), np.sin(fine) * sign, np.cos(coarse), np.sin(coarse) * sign)]


def _x_unit(s, j):
    return SUBS * s + j


def _x_pair(s, j):
    return 64 + SUBS * lax.rem(s, 4) + j


def _w_unit(p, k):
    return 96 + 32 * p + k


def _wo_unit(n):
    return 2 * n


def _run_unit(s, j):
    return 32 + SUBS * s + j


def _in_unit(s, j):
    return 96 + SUBS * s + j


def _out_unit(s, j):
    return 160 + SUBS * lax.rem(s, 2) + j


UNITS = 192


def _kernel(x_ref, gain_hbm, cos_f_hbm, sin_f_hbm, cos_c_hbm, sin_c_hbm, wq_ref, wk_ref, wv_ref, wo_ref, out_ref,
            gain_ref, cos_f, sin_f, cos_c, sin_c, mem, y_s, q_s, k_s, v_s, own, seen, top_s, sum_s, mix_s,
            ring_send, ring_recv, pair_send, pair_recv, sum_send, sum_recv, term_send, term_recv, x_sem, small_sem, y_sem, w_sem, wo_sem, credit, pair_phase, ring_phase):
    core, pos, after, before, partner = _where()
    depth = y_s.shape[1]
    heads = q_s.shape[0]
    wide = depth // SUBS
    parts = wide // SIDE
    deep = wide // TALL
    met = _meet((after, before, partner))
    x_loads = []
    for n, here in enumerate(pl.ds(r, ROWS // 4) for r in range(0, ROWS, ROWS // 4)):
        x_loads.append(pltpu.make_async_copy(x_ref.at[here], y_s.at[here], x_sem.at[n]))
    for load in x_loads:
        load.start()
    smalls = ((gain_hbm, gain_ref), (cos_f_hbm, cos_f), (sin_f_hbm, sin_f), (cos_c_hbm, cos_c), (sin_c_hbm, sin_c))
    small_loads = [pltpu.make_async_copy(a, b, small_sem.at[n]) for n, (a, b) in enumerate(smalls)]
    for load in small_loads:
        load.start()
    weights = (wq_ref, wk_ref, wv_ref)

    def w_load(p, j):
        return pltpu.make_async_copy(weights[p].at[pl.ds(deep * j, deep)], mem.at[pl.ds(_w_unit(p, deep * j), deep)], w_sem.at[p, j])

    def ring(s, j):
        return _send(mem.at[_x_unit(s, j)], mem.at[_x_unit(s + 1, j)], ring_send.at[s, j], ring_recv.at[s, j], after)

    def ring_half(s, j):
        return _send(mem.at[pl.ds(_x_unit(s, j), HALF)], mem.at[pl.ds(_x_unit(s + 1, j), HALF)], ring_send.at[s, j], ring_recv.at[s, j], after)

    def pair(s, j):
        return _send(mem.at[_x_unit(s, j)], mem.at[_x_pair(s, j)], pair_send.at[s, j], pair_recv.at[s, j], partner)

    e = HEAD**-0.5 * LOG2E

    def attend_keys(which, device, starts, size, masked):
        here = pl.ds(pl.multiple_of(device * ROWS, ROWS), ROWS)
        keys = [pl.ds(pl.multiple_of(start, size), size) for start in starts]
        scores = [_dot(jnp.concatenate([k_s[h, part, :] for part in keys], axis=0), q_s[h, here, :], 1, 1) for h in range(heads)]
        if masked:
            gap = lax.broadcasted_iota(jnp.int32, (size, ROWS), 1) - lax.broadcasted_iota(jnp.int32, (size, ROWS), 0)
            ok = jnp.concatenate([gap - start for start in starts], axis=0) >= -device * ROWS
            scores = [jnp.where(ok, t, HIDDEN) for t in scores]
        weights = []
        for h, t in enumerate(scores):
            old = top_s[which, h]
            top = jnp.maximum(old, t.max(axis=0, keepdims=True))
            p = jnp.exp2((t - top) * e)
            keep = jnp.exp2((old - top) * e)
            top_s[which, h] = top
            sum_s[which, h] = sum_s[which, h] * keep + p.sum(axis=0, keepdims=True)
            weights.append((p.astype(jnp.bfloat16), keep))
        for h, (p, keep) in enumerate(weights):
            mix_s[which, h] = mix_s[which, h] * keep + _dot(jnp.concatenate([v_s[h, :, part] for part in keys], axis=1), p)

    def begin(which):
        top_s[which] = jnp.full(top_s.shape[1:], NEG, jnp.float32)
        sum_s[which] = jnp.zeros(sum_s.shape[1:], jnp.float32)
        mix_s[which] = jnp.zeros(mix_s.shape[1:], jnp.float32)

    def finish(s, which):
        for h in range(heads):
            out = (mix_s[which, h] * (1 / sum_s[which, h])).T
            seen[lax.rem(s, 2), which, :, h * HEAD : (h + 1) * HEAD] = out.astype(jnp.bfloat16)

    def block_of(s, which):
        return _owner(pos, s + 1, lax.rem(core + which, 2))

    def attend(s, which):
        device = block_of(s, which)
        begin(which)
        whole = lax.div(device * ROWS, KEYS)
        lax.fori_loop(0, whole, lambda i, _: attend_keys(which, device, [i * KEYS], KEYS, False), None)
        attend_keys(which, device, [whole * KEYS], KEYS, True)
        finish(s, which)

    def ahead(s):
        starts = [_owner(pos, s, parity) * ROWS for parity in range(2)]
        for which in range(2):
            attend_keys(which, block_of(0, which), starts, ROWS, True)

    for n in range(6):
        own[n] = jnp.zeros_like(own[n])
    for which in range(2):
        begin(which)
    group = 16
    scales = []
    for r in range(0, ROWS, group):
        if r % (ROWS // 4) == 0:
            x_loads[r // (ROWS // 4)].wait()
        wide_x = y_s[r : r + group, :].astype(jnp.float32)
        scales.append(lax.rsqrt(jnp.sum(wide_x * wide_x, -1, keepdims=True) * (1 / depth) + 1e-6))
    small_loads[0].wait()
    for j in range(SUBS):
        for i in range(parts):
            here = slice(j * wide + i * SIDE, j * wide + (i + 1) * SIDE)
            gain = gain_ref[here].astype(jnp.float32).reshape(1, SIDE)
            for r in range(0, ROWS, group):
                t = y_s[r : r + group, here].astype(jnp.float32) * scales[r // group] * gain
                mem[_x_unit(0, j), i * ROWS + r : i * ROWS + r + group, :] = t.astype(jnp.bfloat16)
        if j == 0:
            met()
        ring(0, j).start()
        pair(0, j).start()
        for p in range(3):
            w_load(p, j).start()
    for load in small_loads[1:]:
        load.wait()

    def project(t):
        s, j = lax.div(t, SUBS), lax.rem(t, SUBS)
        pair(s, j).wait_recv()
        mine, theirs = _x_unit(s, j), _x_pair(s, j)
        units = mine + core * (theirs - mine), theirs + core * (mine - theirs)
        a = [jnp.concatenate([mem[u, i * ROWS : (i + 1) * ROWS, :] for i in range(parts)], axis=1) for u in units]
        a = jnp.concatenate(a, axis=0)
        for p in range(3):
            @pl.when(s == 0)
            def _():
                w_load(p, j).wait()

            part = _dot(a, mem[pl.ds(_w_unit(p, deep * j), deep)].reshape(wide, SIDE))
            own[p] += part[:ROWS]
            own[3 + p] += part[ROWS:]

        @pl.when(j == SUBS - 1)
        def _():
            for parity in range(2):
                device = _owner(pos, s, parity)
                here = pl.ds(pl.multiple_of(device * ROWS, ROWS), ROWS)
                cf, sf, cc, sc = cos_f[...], sin_f[...], cos_c[device], sin_c[device]
                cos, sin = cc * cf - sc * sf, sc * cf + cc * sf
                for p in range(3):
                    for h in range(heads):
                        t = own[3 * parity + p, :, h * HEAD : (h + 1) * HEAD].astype(jnp.bfloat16).astype(jnp.float32)
                        if p < 2:
                            (q_s, k_s)[p][h, here, :] = (t * cos + pltpu.roll(t, HEAD // 2, 1) * sin).astype(jnp.bfloat16)
                        else:
                            v_s[h, :, here] = t.T.astype(jnp.bfloat16)
            for n in range(6):
                own[n] = jnp.zeros_like(own[n])

            @pl.when(s < 4)
            def _():
                pl.semaphore_signal(credit, inc=1, device_id={"tp": partner}, device_id_type=MESH)

            @pl.when(s == 1)
            def _():
                ahead(0)

            @pl.when(s >= 1)
            def _():
                ahead(s)

    def wo_load(j):
        return [pltpu.make_async_copy(wo_ref.at[:, :, pl.ds((parts * j + i) * SIDE, SIDE)], mem.at[pl.ds(_wo_unit(parts * j + i), 2)], wo_sem.at[j, i])
                for i in range(parts)]

    def arrive(s, j, one, half):
        @pl.when((s == 1) | (s == CHIPS - 1))
        def _():
            one(s - 1, j).wait_recv()

        @pl.when((s > 1) & (s < CHIPS - 1) & (lax.rem(j, HALF) == 0))
        def _():
            half(s - 1, j).wait_recv()

    def depart(s, one, half):
        @pl.when((s == 0) | (s == CHIPS - 2))
        def _():
            for j in range(SUBS):
                one(s, j).wait_send()

        @pl.when((s > 0) & (s < CHIPS - 2))
        def _():
            for j in range(0, SUBS, HALF):
                half(s, j).wait_send()

    def gather(t, _):
        @pl.when((t >= SUBS) & (t < CHIPS * SUBS))
        def _():
            s, j = lax.div(t, SUBS), lax.rem(t, SUBS)
            arrive(s, j, ring, ring_half)

            @pl.when(s == CHIPS - 2)
            def _():
                ring(s, j).start()

            @pl.when((s == 1) & (lax.rem(j, HALF) == HALF - 1))
            def _():
                ring_half(s, j - HALF + 1).start()

            @pl.when((s > 1) & (s < CHIPS - 2) & (lax.rem(j, HALF) == 0))
            def _():
                ring_half(s, j).start()

            @pl.when((s >= 4) & (j == 0))
            def _():
                pl.semaphore_wait(credit, 1)

            pair(s, j).start()

        project(t - 1)

        def sent(s, _):
            depart(s, ring, ring_half)
            for j in range(SUBS):
                pair(s, j).wait_send()

        @pl.when(t == 6 * SUBS)
        def _():
            lax.fori_loop(0, 4, sent, None)
            for j in range(SUBS):
                for load in wo_load(j):
                    load.start()

        @pl.when(t == 7 * SUBS)
        def _():
            lax.fori_loop(4, 6, sent, None)
            for j in range(SUBS):
                pair(6, j).wait_send()

        @pl.when(t > 7 * SUBS)
        def _():
            j = t - 1 - 7 * SUBS
            ring(6, j).wait_send()
            pair(7, j).wait_send()

    lax.fori_loop(1, CHIPS * SUBS + 1, gather, None)
    for semaphore, device in ((pair_phase, partner), (ring_phase, before)):
        pl.semaphore_signal(semaphore, inc=1, device_id={"tp": device}, device_id_type=MESH)
    for load in x_loads:
        load.start()
    def total(s, j):
        return _send(mem.at[_run_unit(s, j)], mem.at[_run_unit(s + 1, j)], sum_send.at[s, j], sum_recv.at[s, j], after)

    def total_half(s, j):
        return _send(mem.at[pl.ds(_run_unit(s, j), HALF)], mem.at[pl.ds(_run_unit(s + 1, j), HALF)], sum_send.at[s, j], sum_recv.at[s, j], after)

    def term(s, j):
        return _send(mem.at[_out_unit(s, j)], mem.at[_in_unit(s, j)], term_send.at[s, j], term_recv.at[s, j], partner)

    def terms(s, j):
        both = seen[lax.rem(s, 2)].reshape(2 * ROWS, heads * HEAD)
        for i in range(parts):
            t = _dot(both, mem[pl.ds(_wo_unit(parts * j + i), 2)].reshape(heads * HEAD, SIDE))
            own[parts * j + i] = t[:ROWS]
            mem[_out_unit(s, j), i * ROWS : (i + 1) * ROWS, :] = t[ROWS:].astype(jnp.bfloat16)
        term(s, j).start()

    strip = 64

    def add(s, j, running, last):
        def some(g, _):
            i, r = lax.div(g, ROWS // strip), pl.multiple_of(lax.rem(g, ROWS // strip) * strip, strip)
            here = pl.ds(pl.multiple_of(g * strip, strip), strip)
            t = own[parts * j + i, pl.ds(r, strip), :] + mem[_in_unit(s, j), here, :].astype(jnp.float32)
            if running:
                t = t + mem[_run_unit(s, j), here, :].astype(jnp.float32)
            if last:
                columns = pl.ds(pl.multiple_of(j * wide + i * SIDE, SIDE), SIDE)
                y_s[pl.ds(r, strip), columns] = (y_s[pl.ds(r, strip), columns].astype(jnp.float32) + t).astype(jnp.bfloat16)
            else:
                mem[_run_unit(s, j), here, :] = t.astype(jnp.bfloat16)

        lax.fori_loop(0, parts * ROWS // strip, some, None)

    def leave(j):
        columns = pl.ds(pl.multiple_of(j * wide, wide), wide)
        return pltpu.make_async_copy(y_s.at[:, columns], out_ref.at[:, columns], y_sem.at[j])

    def first(j, _):
        term(0, j).wait_recv()
        add(0, j, False, False)
        total(0, j).start()

    for which in range(2):
        finish(0, which)
    for j in range(SUBS):
        for load in wo_load(j):
            load.wait()
    pl.semaphore_wait(pair_phase, 1)
    lax.fori_loop(0, SUBS, lambda j, _: terms(0, j), None)
    pl.semaphore_wait(ring_phase, 1)
    lax.fori_loop(0, SUBS, first, None)
    lax.fori_loop(0, 2, lambda i, _: attend(1, i), None)
    lax.fori_loop(0, SUBS, lambda j, _: terms(1, j), None)
    lax.fori_loop(0, 2, lambda i, _: attend(2, i), None)
    for load in x_loads:
        load.wait()

    def scatter(t, _):
        s, j = lax.div(t, SUBS), lax.rem(t, SUBS)
        arrive(s, j, total, total_half)
        term(s, j).wait_recv()

        @pl.when(s < CHIPS - 1)
        def _():
            add(s, j, True, False)

            @pl.when(s == CHIPS - 2)
            def _():
                total(s, j).start()

            @pl.when((s < CHIPS - 2) & (lax.rem(j, HALF) == HALF - 1))
            def _():
                total_half(s, j - HALF + 1).start()

            term(s - 1, j).wait_send()
            terms(s + 1, j)

        @pl.when(s == CHIPS - 1)
        def _():
            add(s, j, True, True)
            leave(j).start()
            total(s - 1, j).wait_send()
            term(s - 1, j).wait_send()
            term(s, j).wait_send()

        @pl.when(t == (CHIPS - 1) * SUBS - 1)
        def _():
            lax.fori_loop(0, CHIPS - 2, lambda s, _: depart(s, total, total_half), None)

        @pl.when((s < CHIPS - 2) & (lax.rem(j, HALF) == HALF - 1))
        def _():
            attend(s + 2, lax.div(j, HALF))

    lax.fori_loop(SUBS, CHIPS * SUBS, scatter, None)

    for j in range(SUBS):
        leave(j).wait()


def _settle(a_ref, b_ref, held, in_sem, out_sem):
    size = held.shape[1]
    ins = [pltpu.make_async_copy(a_ref.at[pl.ds(n * size, size)], held.at[n], in_sem.at[n]) for n in range(held.shape[0])]
    outs = [pltpu.make_async_copy(held.at[n], b_ref.at[pl.ds(n * size, size)], out_sem.at[n]) for n in range(held.shape[0])]
    for copy in ins:
        copy.start()
    for copy, onward in zip(ins, outs):
        copy.wait()
        onward.start()
    for copy in outs:
        copy.wait()


def _settled(y):
    rows, depth = y.shape
    there = pl.BlockSpec(memory_space=pl.ANY)
    return pl.pallas_call(
        _settle,
        out_shape=jax.ShapeDtypeStruct(y.shape, y.dtype),
        in_specs=[there],
        out_specs=there,
        scratch_shapes=[pltpu.VMEM((8, rows // 8, depth), y.dtype), pltpu.SemaphoreType.DMA((8,)), pltpu.SemaphoreType.DMA((8,))],
        compiler_params=pltpu.CompilerParams(vmem_limit_bytes=VMEM),
        cost_estimate=pl.CostEstimate(flops=0, bytes_accessed=4 * rows * depth, transcendentals=0),
        name="settle",
    )(y)


def solution(mesh):
    def step(x, gain, wq, wk, wv, wo):
        depth, cols = wq.shape
        heads, tokens = cols // HEAD, 2 * CHIPS * ROWS
        there = pl.BlockSpec(memory_space=pl.ANY)
        low = jnp.bfloat16
        y = pl.pallas_call(
            _kernel,
            out_shape=jax.ShapeDtypeStruct((ROWS, depth), low),
            in_specs=[there] * 10,
            out_specs=there,
            scratch_shapes=[
                pltpu.VMEM((depth,), low),
                *[pltpu.VMEM((ROWS, HEAD), jnp.float32)] * 2,
                *[pltpu.VMEM((2 * CHIPS, 1, HEAD), jnp.float32)] * 2,
                pltpu.VMEM((UNITS, TALL, SIDE), low),
                pltpu.VMEM((ROWS, depth), low),
                pltpu.VMEM((heads, tokens, HEAD), low),
                pltpu.VMEM((heads, tokens, HEAD), low),
                pltpu.VMEM((heads, HEAD, tokens), low),
                pltpu.VMEM((depth // SIDE, ROWS, SIDE), jnp.float32),
                pltpu.VMEM((2, 2, ROWS, cols), low),
                pltpu.VMEM((2, heads, 1, ROWS), jnp.float32),
                pltpu.VMEM((2, heads, 1, ROWS), jnp.float32),
                pltpu.VMEM((2, heads, HEAD, ROWS), jnp.float32),
                *[pltpu.SemaphoreType.DMA((CHIPS - 1, SUBS))] * 2,
                *[pltpu.SemaphoreType.DMA((CHIPS, SUBS))] * 2,
                *[pltpu.SemaphoreType.DMA((CHIPS - 1, SUBS))] * 2,
                *[pltpu.SemaphoreType.DMA((CHIPS, SUBS))] * 2,
                pltpu.SemaphoreType.DMA((4,)),
                pltpu.SemaphoreType.DMA((5,)),
                pltpu.SemaphoreType.DMA((SUBS,)),
                pltpu.SemaphoreType.DMA((3, SUBS)),
                pltpu.SemaphoreType.DMA((SUBS, depth // SUBS // SIDE)),
                *[pltpu.SemaphoreType.REGULAR] * 3,
            ],
            compiler_params=pltpu.CompilerParams(collective_id=0, has_side_effects=True, vmem_limit_bytes=VMEM),
            cost_estimate=pl.CostEstimate(flops=8 * tokens * depth * cols, bytes_accessed=8 * depth * cols,
                                          transcendentals=heads * tokens * tokens // 2),
            name="attention_half",
        )(x, gain, *_tables(), *[w.reshape(-1, TALL, cols) for w in (wq, wk, wv)], wo.reshape(-1, TALL, depth))
        return _settled(y)

    tokens, columns = P(("dp", "tp"), None), P(None, "tp")
    return jax.shard_map(
        step,
        mesh=mesh,
        in_specs=(tokens, P(None), columns, columns, columns, P("tp", None)),
        out_specs=tokens,
        check_vma=False,
    )
```

```python
import functools

import jax
import jax.numpy as jnp
import numpy as np
from jax import lax
from jax.experimental import pallas as pl
from jax.experimental.pallas import tpu as pltpu
from jax.sharding import PartitionSpec as P

HEAD = 128
THETA = 10000
NEG = -1e30
HIDDEN = 2 * NEG
LOG2E = 1.4426950408889634
CHIPS = 8
ROWS = 128
SUBS = 8
HALF = SUBS // 2
SIDE = 512
TALL = 256
KEYS = 256
VMEM = 67043328
MESH = pl.DeviceIdType.MESH


def _dot(a, b, ca=1, cb=0):
    return lax.dot_general(a, b, (((ca,), (cb,)), ((), ())), preferred_element_type=jnp.float32)


def _chip(pos):
    return pos + lax.div(pos, 4) * (11 - 2 * pos)


def _where():
    me = lax.axis_index("tp")
    core, chip = lax.rem(me, 2), lax.div(me, 2)
    pos = _chip(chip)
    after = 2 * _chip(lax.rem(pos + 1 + 6 * core, CHIPS)) + core
    before = 2 * _chip(lax.rem(pos + 7 - 6 * core, CHIPS)) + core
    return core, pos, after, before, me + 1 - 2 * core


def _owner(pos, steps, parity):
    return 2 * _chip(lax.rem(pos + steps * (7 - 6 * parity), CHIPS)) + parity


def _meet(devices):
    barrier = pltpu.get_barrier_semaphore()
    for device in devices:
        pl.semaphore_signal(barrier, inc=1, device_id={"tp": device}, device_id_type=MESH)
    return lambda: pl.semaphore_wait(barrier, len(devices))


def _send(src, dst, send_sem, recv_sem, device):
    return pltpu.make_async_remote_copy(src_ref=src, dst_ref=dst, send_sem=send_sem, recv_sem=recv_sem, device_id={"tp": device},
                                        device_id_type=MESH)


def _tables():
    rate = np.tile(float(THETA) ** (-np.arange(HEAD // 2) / (HEAD // 2)), 2)
    sign = np.where(np.arange(HEAD) < HEAD // 2, -1.0, 1.0)
    fine, coarse = np.arange(ROWS)[:, None] * rate, (np.arange(2 * CHIPS) * ROWS)[:, None, None] * rate
    return [jnp.asarray(t, jnp.float32) for t in (np.cos(fine), np.sin(fine) * sign, np.cos(coarse), np.sin(coarse) * sign)]


def _x_unit(s, j):
    return SUBS * s + j


def _x_pair(s, j):
    return 64 + SUBS * lax.rem(s, 4) + j


def _w_unit(p, k):
    return 96 + 32 * p + k


def _wo_unit(n):
    return 2 * n


def _run_unit(s, j):
    return 32 + SUBS * s + j


def _in_unit(s, j):
    return 96 + SUBS * s + j


def _out_unit(s, j):
    return 160 + SUBS * lax.rem(s, 2) + j


UNITS = 192


def _kernel(x_ref, gain_hbm, cos_f_hbm, sin_f_hbm, cos_c_hbm, sin_c_hbm, wq_ref, wk_ref, wv_ref, wo_ref, out_ref,
            gain_ref, cos_f, sin_f, cos_c, sin_c, mem, y_s, q_s, k_s, v_s, own, seen, top_s, sum_s, mix_s,
            ring_send, ring_recv, pair_send, pair_recv, sum_send, sum_recv, term_send, term_recv, x_sem, small_sem, y_sem, w_sem, wo_sem, credit, pair_phase, ring_phase):
    core, pos, after, before, partner = _where()
    depth = y_s.shape[1]
    heads = q_s.shape[0]
    wide = depth // SUBS
    parts = wide // SIDE
    deep = wide // TALL
    met = _meet((after, before, partner))
    x_loads = []
    for n, here in enumerate(pl.ds(r, ROWS // 4) for r in range(0, ROWS, ROWS // 4)):
        x_loads.append(pltpu.make_async_copy(x_ref.at[here], y_s.at[here], x_sem.at[n]))
    for load in x_loads:
        load.start()
    smalls = ((gain_hbm, gain_ref), (cos_f_hbm, cos_f), (sin_f_hbm, sin_f), (cos_c_hbm, cos_c), (sin_c_hbm, sin_c))
    small_loads = [pltpu.make_async_copy(a, b, small_sem.at[n]) for n, (a, b) in enumerate(smalls)]
    for load in small_loads:
        load.start()
    weights = (wq_ref, wk_ref, wv_ref)

    def w_load(p, j):
        return pltpu.make_async_copy(weights[p].at[pl.ds(deep * j, deep)], mem.at[pl.ds(_w_unit(p, deep * j), deep)], w_sem.at[p, j])

    def ring(s, j):
        return _send(mem.at[_x_unit(s, j)], mem.at[_x_unit(s + 1, j)], ring_send.at[s, j], ring_recv.at[s, j], after)

    def ring_half(s, j):
        return _send(mem.at[pl.ds(_x_unit(s, j), HALF)], mem.at[pl.ds(_x_unit(s + 1, j), HALF)], ring_send.at[s, j], ring_recv.at[s, j], after)

    def pair(s, j):
        return _send(mem.at[_x_unit(s, j)], mem.at[_x_pair(s, j)], pair_send.at[s, j], pair_recv.at[s, j], partner)

    e = HEAD**-0.5 * LOG2E

    def attend_keys(which, device, starts, size, masked):
        here = pl.ds(pl.multiple_of(device * ROWS, ROWS), ROWS)
        keys = [pl.ds(pl.multiple_of(start, size), size) for start in starts]
        scores = [_dot(jnp.concatenate([k_s[h, part, :] for part in keys], axis=0), q_s[h, here, :], 1, 1) for h in range(heads)]
        if masked:
            gap = lax.broadcasted_iota(jnp.int32, (size, ROWS), 1) - lax.broadcasted_iota(jnp.int32, (size, ROWS), 0)
            ok = jnp.concatenate([gap - start for start in starts], axis=0) >= -device * ROWS
            scores = [jnp.where(ok, t, HIDDEN) for t in scores]
        weights = []
        for h, t in enumerate(scores):
            old = top_s[which, h]
            top = jnp.maximum(old, t.max(axis=0, keepdims=True))
            p = jnp.exp2((t - top) * e)
            keep = jnp.exp2((old - top) * e)
            top_s[which, h] = top
            sum_s[which, h] = sum_s[which, h] * keep + p.sum(axis=0, keepdims=True)
            weights.append((p.astype(jnp.bfloat16), keep))
        for h, (p, keep) in enumerate(weights):
            mix_s[which, h] = mix_s[which, h] * keep + _dot(jnp.concatenate([v_s[h, :, part] for part in keys], axis=1), p)

    def begin(which):
        top_s[which] = jnp.full(top_s.shape[1:], NEG, jnp.float32)
        sum_s[which] = jnp.zeros(sum_s.shape[1:], jnp.float32)
        mix_s[which] = jnp.zeros(mix_s.shape[1:], jnp.float32)

    def finish(s, which):
        for h in range(heads):
            out = (mix_s[which, h] * (1 / sum_s[which, h])).T
            seen[lax.rem(s, 2), which, :, h * HEAD : (h + 1) * HEAD] = out.astype(jnp.bfloat16)

    def block_of(s, which):
        return _owner(pos, s + 1, lax.rem(core + which, 2))

    def attend(s, which):
        device = block_of(s, which)
        begin(which)
        whole = lax.div(device * ROWS, KEYS)
        lax.fori_loop(0, whole, lambda i, _: attend_keys(which, device, [i * KEYS], KEYS, False), None)
        attend_keys(which, device, [whole * KEYS], KEYS, True)
        finish(s, which)

    def ahead(s):
        starts = [_owner(pos, s, parity) * ROWS for parity in range(2)]
        for which in range(2):
            attend_keys(which, block_of(0, which), starts, ROWS, True)

    for n in range(6):
        own[n] = jnp.zeros_like(own[n])
    for which in range(2):
        begin(which)
    group = 16
    scales = []
    for r in range(0, ROWS, group):
        if r % (ROWS // 4) == 0:
            x_loads[r // (ROWS // 4)].wait()
        wide_x = y_s[r : r + group, :].astype(jnp.float32)
        scales.append(lax.rsqrt(jnp.sum(wide_x * wide_x, -1, keepdims=True) * (1 / depth) + 1e-6))
    small_loads[0].wait()
    for j in range(SUBS):
        for i in range(parts):
            here = slice(j * wide + i * SIDE, j * wide + (i + 1) * SIDE)
            gain = gain_ref[here].astype(jnp.float32).reshape(1, SIDE)
            for r in range(0, ROWS, group):
                t = y_s[r : r + group, here].astype(jnp.float32) * scales[r // group] * gain
                mem[_x_unit(0, j), i * ROWS + r : i * ROWS + r + group, :] = t.astype(jnp.bfloat16)
        if j == 0:
            met()
        ring(0, j).start()
        pair(0, j).start()
        for p in range(3):
            w_load(p, j).start()
    for load in small_loads[1:]:
        load.wait()

    def project(t):
        s, j = lax.div(t, SUBS), lax.rem(t, SUBS)
        pair(s, j).wait_recv()
        mine, theirs = _x_unit(s, j), _x_pair(s, j)
        units = mine + core * (theirs - mine), theirs + core * (mine - theirs)
        a = [jnp.concatenate([mem[u, i * ROWS : (i + 1) * ROWS, :] for i in range(parts)], axis=1) for u in units]
        a = jnp.concatenate(a, axis=0)
        for p in range(3):
            @pl.when(s == 0)
            def _():
                w_load(p, j).wait()

            part = _dot(a, mem[pl.ds(_w_unit(p, deep * j), deep)].reshape(wide, SIDE))
            own[p] += part[:ROWS]
            own[3 + p] += part[ROWS:]

        @pl.when(j == SUBS - 1)
        def _():
            for parity in range(2):
                device = _owner(pos, s, parity)
                here = pl.ds(pl.multiple_of(device * ROWS, ROWS), ROWS)
                cf, sf, cc, sc = cos_f[...], sin_f[...], cos_c[device], sin_c[device]
                cos, sin = cc * cf - sc * sf, sc * cf + cc * sf
                for p in range(3):
                    for h in range(heads):
                        t = own[3 * parity + p, :, h * HEAD : (h + 1) * HEAD].astype(jnp.bfloat16).astype(jnp.float32)
                        if p < 2:
                            (q_s, k_s)[p][h, here, :] = (t * cos + pltpu.roll(t, HEAD // 2, 1) * sin).astype(jnp.bfloat16)
                        else:
                            v_s[h, :, here] = t.T.astype(jnp.bfloat16)
            for n in range(6):
                own[n] = jnp.zeros_like(own[n])

            @pl.when(s < 4)
            def _():
                pl.semaphore_signal(credit, inc=1, device_id={"tp": partner}, device_id_type=MESH)

            @pl.when(s == 1)
            def _():
                ahead(0)

            @pl.when(s >= 1)
            def _():
                ahead(s)

    def wo_load(j):
        return [pltpu.make_async_copy(wo_ref.at[:, :, pl.ds((parts * j + i) * SIDE, SIDE)], mem.at[pl.ds(_wo_unit(parts * j + i), 2)], wo_sem.at[j, i])
                for i in range(parts)]

    def arrive(s, j, one, half):
        @pl.when((s == 1) | (s == CHIPS - 1))
        def _():
            one(s - 1, j).wait_recv()

        @pl.when((s > 1) & (s < CHIPS - 1) & (lax.rem(j, HALF) == 0))
        def _():
            half(s - 1, j).wait_recv()

    def depart(s, one, half):
        @pl.when((s == 0) | (s == CHIPS - 2))
        def _():
            for j in range(SUBS):
                one(s, j).wait_send()

        @pl.when((s > 0) & (s < CHIPS - 2))
        def _():
            for j in range(0, SUBS, HALF):
                half(s, j).wait_send()

    def gather(t, _):
        @pl.when((t >= SUBS) & (t < CHIPS * SUBS))
        def _():
            s, j = lax.div(t, SUBS), lax.rem(t, SUBS)
            arrive(s, j, ring, ring_half)

            @pl.when(s == CHIPS - 2)
            def _():
                ring(s, j).start()

            @pl.when((s == 1) & (lax.rem(j, HALF) == HALF - 1))
            def _():
                ring_half(s, j - HALF + 1).start()

            @pl.when((s > 1) & (s < CHIPS - 2) & (lax.rem(j, HALF) == 0))
            def _():
                ring_half(s, j).start()

            @pl.when((s >= 4) & (j == 0))
            def _():
                pl.semaphore_wait(credit, 1)

            pair(s, j).start()

        project(t - 1)

        def sent(s, _):
            depart(s, ring, ring_half)
            for j in range(SUBS):
                pair(s, j).wait_send()

        @pl.when(t == 6 * SUBS)
        def _():
            lax.fori_loop(0, 4, sent, None)
            for j in range(SUBS):
                for load in wo_load(j):
                    load.start()

        @pl.when(t == 7 * SUBS)
        def _():
            lax.fori_loop(4, 6, sent, None)
            for j in range(SUBS):
                pair(6, j).wait_send()
                for load in wo_load(j):
                    load.wait()
            for load in x_loads:
                load.start()

        @pl.when(t > 7 * SUBS)
        def _():
            j = t - 1 - 7 * SUBS
            ring(6, j).wait_send()
            pair(7, j).wait_send()

    lax.fori_loop(1, CHIPS * SUBS + 1, gather, None)
    for semaphore, device in ((pair_phase, partner), (ring_phase, before)):
        pl.semaphore_signal(semaphore, inc=1, device_id={"tp": device}, device_id_type=MESH)
    def total(s, j):
        return _send(mem.at[_run_unit(s, j)], mem.at[_run_unit(s + 1, j)], sum_send.at[s, j], sum_recv.at[s, j], after)

    def total_half(s, j):
        return _send(mem.at[pl.ds(_run_unit(s, j), HALF)], mem.at[pl.ds(_run_unit(s + 1, j), HALF)], sum_send.at[s, j], sum_recv.at[s, j], after)

    def term(s, j):
        return _send(mem.at[_out_unit(s, j)], mem.at[_in_unit(s, j)], term_send.at[s, j], term_recv.at[s, j], partner)

    def terms(s, j):
        both = seen[lax.rem(s, 2)].reshape(2 * ROWS, heads * HEAD)
        for i in range(parts):
            t = _dot(both, mem[pl.ds(_wo_unit(parts * j + i), 2)].reshape(heads * HEAD, SIDE))
            own[parts * j + i] = t[:ROWS]
            mem[_out_unit(s, j), i * ROWS : (i + 1) * ROWS, :] = t[ROWS:].astype(jnp.bfloat16)

        @pl.when((s == 0) & (j == 0))
        def _():
            pl.semaphore_wait(pair_phase, 1)

        term(s, j).start()

    strip = 64

    def add(s, j, running, last):
        def some(g, _):
            i, r = lax.div(g, ROWS // strip), pl.multiple_of(lax.rem(g, ROWS // strip) * strip, strip)
            here = pl.ds(pl.multiple_of(g * strip, strip), strip)
            t = own[parts * j + i, pl.ds(r, strip), :] + mem[_in_unit(s, j), here, :].astype(jnp.float32)
            if running:
                t = t + mem[_run_unit(s, j), here, :].astype(jnp.float32)
            if last:
                columns = pl.ds(pl.multiple_of(j * wide + i * SIDE, SIDE), SIDE)
                y_s[pl.ds(r, strip), columns] = (y_s[pl.ds(r, strip), columns].astype(jnp.float32) + t).astype(jnp.bfloat16)
            else:
                mem[_run_unit(s, j), here, :] = t.astype(jnp.bfloat16)

        lax.fori_loop(0, parts * ROWS // strip, some, None)

    def leave(j):
        columns = pl.ds(pl.multiple_of(j * wide, wide), wide)
        return pltpu.make_async_copy(y_s.at[:, columns], out_ref.at[:, columns], y_sem.at[j])

    def first(j, _):
        term(0, j).wait_recv()
        add(0, j, False, False)
        total(0, j).start()

    for which in range(2):
        finish(0, which)
    lax.fori_loop(0, SUBS, lambda j, _: terms(0, j), None)
    pl.semaphore_wait(ring_phase, 1)
    lax.fori_loop(0, SUBS, first, None)
    lax.fori_loop(0, 2, lambda i, _: attend(1, i), None)
    lax.fori_loop(0, SUBS, lambda j, _: terms(1, j), None)
    lax.fori_loop(0, 2, lambda i, _: attend(2, i), None)
    for load in x_loads:
        load.wait()

    def scatter(t, _):
        s, j = lax.div(t, SUBS), lax.rem(t, SUBS)
        arrive(s, j, total, total_half)
        term(s, j).wait_recv()

        @pl.when(s < CHIPS - 1)
        def _():
            add(s, j, True, False)

            @pl.when(s == CHIPS - 2)
            def _():
                total(s, j).start()

            @pl.when((s < CHIPS - 2) & (lax.rem(j, HALF) == HALF - 1))
            def _():
                total_half(s, j - HALF + 1).start()

            term(s - 1, j).wait_send()
            terms(s + 1, j)

        @pl.when(s == CHIPS - 1)
        def _():
            add(s, j, True, True)
            leave(j).start()
            total(s - 1, j).wait_send()
            term(s - 1, j).wait_send()
            term(s, j).wait_send()

        @pl.when(t == (CHIPS - 1) * SUBS - 1)
        def _():
            lax.fori_loop(0, CHIPS - 2, lambda s, _: depart(s, total, total_half), None)

        @pl.when((s < CHIPS - 2) & (lax.rem(j, HALF) == HALF - 1))
        def _():
            attend(s + 2, lax.div(j, HALF))

    lax.fori_loop(SUBS, CHIPS * SUBS, scatter, None)

    for j in range(SUBS):
        leave(j).wait()


def _settle(a_ref, b_ref, held, in_sem, out_sem):
    size = held.shape[1]
    ins = [pltpu.make_async_copy(a_ref.at[pl.ds(n * size, size)], held.at[n], in_sem.at[n]) for n in range(held.shape[0])]
    outs = [pltpu.make_async_copy(held.at[n], b_ref.at[pl.ds(n * size, size)], out_sem.at[n]) for n in range(held.shape[0])]
    for copy in ins:
        copy.start()
    for copy, onward in zip(ins, outs):
        copy.wait()
        onward.start()
    for copy in outs:
        copy.wait()


def _settled(y):
    rows, depth = y.shape
    there = pl.BlockSpec(memory_space=pl.ANY)
    return pl.pallas_call(
        _settle,
        out_shape=jax.ShapeDtypeStruct(y.shape, y.dtype),
        in_specs=[there],
        out_specs=there,
        scratch_shapes=[pltpu.VMEM((8, rows // 8, depth), y.dtype), pltpu.SemaphoreType.DMA((8,)), pltpu.SemaphoreType.DMA((8,))],
        compiler_params=pltpu.CompilerParams(vmem_limit_bytes=VMEM),
        cost_estimate=pl.CostEstimate(flops=0, bytes_accessed=4 * rows * depth, transcendentals=0),
        name="settle",
    )(y)


def solution(mesh):
    def step(x, gain, wq, wk, wv, wo):
        depth, cols = wq.shape
        heads, tokens = cols // HEAD, 2 * CHIPS * ROWS
        there = pl.BlockSpec(memory_space=pl.ANY)
        low = jnp.bfloat16
        y = pl.pallas_call(
            _kernel,
            out_shape=jax.ShapeDtypeStruct((ROWS, depth), low),
            in_specs=[there] * 10,
            out_specs=there,
            scratch_shapes=[
                pltpu.VMEM((depth,), low),
                *[pltpu.VMEM((ROWS, HEAD), jnp.float32)] * 2,
                *[pltpu.VMEM((2 * CHIPS, 1, HEAD), jnp.float32)] * 2,
                pltpu.VMEM((UNITS, TALL, SIDE), low),
                pltpu.VMEM((ROWS, depth), low),
                pltpu.VMEM((heads, tokens, HEAD), low),
                pltpu.VMEM((heads, tokens, HEAD), low),
                pltpu.VMEM((heads, HEAD, tokens), low),
                pltpu.VMEM((depth // SIDE, ROWS, SIDE), jnp.float32),
                pltpu.VMEM((2, 2, ROWS, cols), low),
                pltpu.VMEM((2, heads, 1, ROWS), jnp.float32),
                pltpu.VMEM((2, heads, 1, ROWS), jnp.float32),
                pltpu.VMEM((2, heads, HEAD, ROWS), jnp.float32),
                *[pltpu.SemaphoreType.DMA((CHIPS - 1, SUBS))] * 2,
                *[pltpu.SemaphoreType.DMA((CHIPS, SUBS))] * 2,
                *[pltpu.SemaphoreType.DMA((CHIPS - 1, SUBS))] * 2,
                *[pltpu.SemaphoreType.DMA((CHIPS, SUBS))] * 2,
                pltpu.SemaphoreType.DMA((4,)),
                pltpu.SemaphoreType.DMA((5,)),
                pltpu.SemaphoreType.DMA((SUBS,)),
                pltpu.SemaphoreType.DMA((3, SUBS)),
                pltpu.SemaphoreType.DMA((SUBS, depth // SUBS // SIDE)),
                *[pltpu.SemaphoreType.REGULAR] * 3,
            ],
            compiler_params=pltpu.CompilerParams(collective_id=0, has_side_effects=True, vmem_limit_bytes=VMEM),
            cost_estimate=pl.CostEstimate(flops=8 * tokens * depth * cols, bytes_accessed=8 * depth * cols,
                                          transcendentals=heads * tokens * tokens // 2),
            name="attention_half",
        )(x, gain, *_tables(), *[w.reshape(-1, TALL, cols) for w in (wq, wk, wv)], wo.reshape(-1, TALL, depth))
        return _settled(y)

    tokens, columns = P(("dp", "tp"), None), P(None, "tp")
    return jax.shard_map(
        step,
        mesh=mesh,
        in_specs=(tokens, P(None), columns, columns, columns, P("tp", None)),
        out_specs=tokens,
        check_vma=False,
    )
```
